256 devices in a mesh: win: 2 (over y), px: 128 (over x, z, core).
Axes of the slice: x: 4, y: 2, z: 16, core: 2. Of those that a mesh axis runs over, the one named last changes fastest.
The devices are a block of a 4x16x16 slice.
Arguments:
- charge_a: float32 [1048576], P(('win', 'px')), parts along dimension 0, may hold values from -3 to 3
- charge_b: float32 [1048576], P(('win', 'px')), parts along dimension 0, may hold values from -3 to 3
- coupling: float32 [2], P('win'), parts along dimension 0, may hold values from 0.1 to 0.9
- positions: float32 [3, 1048576], P(None, ('win', 'px')), parts along dimension 1, may hold values from 0 to 128, as said below
- grid_base: int32 [3, 1048576], P(None, ('win', 'px')), parts along dimension 1, may hold values from 0 to 127, as said below
- spline: float32 [3, 4, 1048576], P(None, None, ('win', 'px')), parts along dimension 2, may hold values from 0 to 0.67, as said below
- spline_slope: float32 [3, 4, 1048576], P(None, None, ('win', 'px')), parts along dimension 2, may hold values from -0.67 to 0.67, as said below
- influence: float32 [128, 128, 128], P(None, 'px'), may hold values from 0.5 to 300, as said below
- pair_tiles: int32 [8192, 12], P(('win', 'px')), parts along dimension 0, may hold values from 0 to 39
- ghost_lists: int32 [2, 131072], P(None, ('win', 'px')), parts along dimension 1, may hold values from 0 to 4095
Outputs:
- forces: float32 [3, 1048576], P(None, ('win', 'px')), parts along dimension 1
The draws below stay inside these ranges and needn't reach their ends.
There are 2 independent parts, one for each index of `win`. The reference program is written for one: setup_inputs(seed, part) draws one part's arguments, and reference() takes and returns one part's arrays. A program takes and returns all parts, laid end to end along the dimension named above; an argument that names none is the same for every part. Nothing has to cross between parts.
Inputs may be any that keep to these rules, and one draw needn't show every extreme that they name: `grid_base`: row 0 of atom i lies in [d, (d + 1)) for d = i // 4096; rows 1 and 2 lie in [0, 128). `positions`: row 0 of atom i lies in [d, (d + 1)) for d = i // 4096; rows 1 and 2 lie in [0, 8). For each atom and dimension, the 4 cubic B-spline weights at some fraction u in [0, 1). `spline_slope`: the derivatives in u of the weights in spline, at the same u. influence at wave index m equals influence at -m, indices taken modulo the grid's lengths.
All inputs are finite; a program needn't handle non-finite values.
Results may differ from the reference program's by a relative error of at most 0.0003.
Values sent between devices are 32-bit elements; how exact they have to be, the bound alone decides.
A program may use at most 128 MiB of HBM per device.

```python
import math
import jax
import jax.numpy as jnp
from jax import lax

KX = 128
KY = 128
KZ = 128
ORDER = 4
TILE = 128
NBR = 12
ATOMS_DEV = 4096
GH_DEV = 512
PLANES = 1
ATOMS = 524288
GHOSTS = 65536
N_PX = 128


def draw_grid_base(key, part):
    key_x, key_y, key_z = jax.random.split(jax.random.fold_in(key, 11), 3)
    atom_ids = jnp.arange(ATOMS, dtype=jnp.int32)
    slab_start = atom_ids // ATOMS_DEV * PLANES
    row_x = slab_start + jax.random.randint(key_x, (ATOMS,), 0, PLANES, dtype=jnp.int32)
    row_y = jax.random.randint(key_y, (ATOMS,), 0, KY, dtype=jnp.int32)
    row_z = jax.random.randint(key_z, (ATOMS,), 0, KZ, dtype=jnp.int32)
    return jnp.stack([row_x, row_y, row_z]).astype(jnp.int32)


def spline_fraction(key):
    return jax.random.uniform(jax.random.fold_in(key, 23), (3, ATOMS), jnp.float32)


def draw_spline(key, part):
    fraction = spline_fraction(key)
    remain = 1.0 - fraction
    cube = fraction * fraction * fraction
    square = fraction * fraction
    weights = [remain * remain * remain / 6.0, (3.0 * cube - 6.0 * square + 4.0) / 6.0, (-3.0 * cube + 3.0 * square + 3.0 * fraction + 1.0) / 6.0, cube / 6.0]
    return jnp.stack(weights, axis=1).astype(jnp.float32)


def draw_spline_slope(key, part):
    fraction = spline_fraction(key)
    remain = 1.0 - fraction
    square = fraction * fraction
    slopes = [-remain * remain / 2.0, (3.0 * square - 4.0 * fraction) / 2.0, (-3.0 * square + 2.0 * fraction + 1.0) / 2.0, square / 2.0]
    return jnp.stack(slopes, axis=1).astype(jnp.float32)


def draw_positions(key, part):
    key_x, key_y = jax.random.split(jax.random.fold_in(key, 37), 2)
    atom_ids = jnp.arange(ATOMS, dtype=jnp.int32)
    slab_start = (atom_ids // ATOMS_DEV * PLANES).astype(jnp.float32)
    inside = jax.random.uniform(key_x, (ATOMS,), jnp.float32)
    across = 8.0 * jax.random.uniform(key_y, (2, ATOMS), jnp.float32)
    row_x = slab_start + PLANES * inside * 0.999
    return jnp.concatenate([row_x[None], across * 0.999], axis=0).astype(jnp.float32)


def draw_influence(key, part):
    lowest, highest = (1.0, 100.0)
    exponent = jax.random.uniform(jax.random.fold_in(key, 53), (KX, KY, KZ), jnp.float32, jnp.log(lowest), jnp.log(highest))
    base_field = jnp.exp(exponent)
    mirror = jnp.roll(jnp.flip(base_field, axis=(0, 1, 2)), 1, axis=(0, 1, 2))
    return (0.5 * (base_field + mirror)).astype(jnp.float32)


def plant(entries, key, low, high):
    spot = [jax.random.randint(jax.random.fold_in(key, axis), (), 0, length) for axis, length in enumerate(entries.shape)]
    longest = entries.shape.index(max(entries.shape))
    neighbour = spot[:longest] + [(spot[longest] + 1) % entries.shape[longest]] + spot[longest + 1:]
    return entries.at[tuple(spot)].set(low).at[tuple(neighbour)].set(high)


def level_of(rng, shape, cuts, low, largest):
    def one(axis_at, parts):
        steps = jax.random.uniform(jax.random.fold_in(jax.random.fold_in(rng, 6), axis_at), (parts,), jnp.float32, low / len(cuts), largest / len(cuts))
        return jnp.repeat(jnp.exp(steps), shape[axis_at] // parts).reshape((-1,) + (1,) * (len(shape) - axis_at - 1))

    gain = one(*cuts[0])
    for cut in cuts[1:]:
        gain = gain * one(*cut)
    return gain


def scatter_about(key, extent, spread, reach, shards=(), held_as=jnp.bfloat16):
    result = spread * jax.random.normal(key, extent, jnp.float32)
    if shards:
        result = result * level_of(key, extent, shards, -0.22, 0.18)
    return jnp.clip(result, -reach, reach).astype(held_as)


def setup_inputs(seed: int = 0, part: int = 0) -> dict:
    key_of = jax.random.split(jax.random.key(seed), 11)
    own_keys = jax.random.split(jax.random.fold_in(key_of[10], part), 11)
    charge_a = scatter_about(own_keys[0], (ATOMS,), 0.5, 3.0, ((0, 128),), jnp.float32)
    charge_b = scatter_about(own_keys[1], (ATOMS,), 0.5, 3.0, ((0, 128),), jnp.float32)
    coupling = jnp.clip(jax.random.uniform(own_keys[2], (1,), jnp.float32, 0.1, 0.9), 0.1, 0.9)
    positions = draw_positions(jax.random.fold_in(jax.random.fold_in(key_of[10], part), 71), part)
    grid_base = draw_grid_base(jax.random.fold_in(jax.random.fold_in(key_of[10], part), 71), part)
    spline = draw_spline(jax.random.fold_in(jax.random.fold_in(key_of[10], part), 71), part)
    spline_slope = draw_spline_slope(jax.random.fold_in(jax.random.fold_in(key_of[10], part), 71), part)
    influence = draw_influence(jax.random.fold_in(key_of[10], 71), part)
    pair_tiles = plant(jax.random.randint(own_keys[8], (ATOMS // TILE, NBR), 0, (ATOMS_DEV + 2 * GH_DEV) // TILE), jax.random.fold_in(own_keys[8], 1), 0, ((ATOMS_DEV + 2 * GH_DEV) // TILE) - 1).astype(jnp.int32)
    ghost_lists = plant(jax.random.randint(own_keys[9], (2, GHOSTS), 0, ATOMS_DEV), jax.random.fold_in(own_keys[9], 1), 0, ATOMS_DEV - 1).astype(jnp.int32)
    return dict(charge_a=charge_a, charge_b=charge_b, coupling=coupling, positions=positions, grid_base=grid_base, spline=spline, spline_slope=spline_slope, influence=influence, pair_tiles=pair_tiles, ghost_lists=ghost_lists)


ewald_beta = 0.35
soften_sq = 0.25

def pair_block(home_rows, nearby, weight_b):
    separation = home_rows[0:3, :, :, None] - nearby[0:3, :, None, :]
    dist_sq = lax.optimization_barrier(jnp.sum(separation * separation, axis=0)) + soften_sq
    distance = jnp.sqrt(dist_sq)
    radial = (jax.scipy.special.erfc(ewald_beta * distance) / distance + 2.0 * ewald_beta / math.sqrt(math.pi) * jnp.exp(-ewald_beta * ewald_beta * dist_sq)) / dist_sq
    mixed = (1.0 - weight_b) * home_rows[3][:, :, None] * nearby[3][:, None, :] + weight_b * home_rows[4][:, :, None] * nearby[4][:, None, :]
    return lax.optimization_barrier(jnp.sum((mixed * radial)[None] * separation, axis=3))

def device_pairs(home_rows, candidates, tile_list, weight_b):
    home_tiles = home_rows.reshape(5, -1, TILE)
    cand_tiles = candidates.reshape(5, -1, TILE)

    def one_slot(accumulated, column):
        nearby = jnp.take(cand_tiles, column, axis=1)
        return (accumulated + pair_block(home_tiles, nearby, weight_b), None)
    start = jnp.zeros((3,) + home_tiles.shape[1:], jnp.float32)
    accumulated, unused = lax.scan(one_slot, start, tile_list.T)
    return accumulated.reshape(3, -1)

def reference(charge_a, charge_b, coupling, positions, grid_base, spline, spline_slope, influence, pair_tiles, ghost_lists):
    weight_b = coupling[0]
    charges = jnp.stack([charge_a, charge_b])
    charge_grid = jnp.zeros((2, KX, KY, KZ), jnp.float32)
    for offset_x in range(ORDER):
        for offset_y in range(ORDER):
            for offset_z in range(ORDER):
                index_x = (grid_base[0] + offset_x) % KX
                index_y = (grid_base[1] + offset_y) % KY
                index_z = (grid_base[2] + offset_z) % KZ
                weight = spline[0, offset_x] * spline[1, offset_y] * spline[2, offset_z]
                charge_grid = charge_grid.at[:, index_x, index_y, index_z].add(charges * weight[None])
    spectrum = jnp.fft.fftn(charge_grid, axes=(1, 2, 3)) * influence[None]
    potential = jnp.real(jnp.fft.ifftn(spectrum, axes=(1, 2, 3))).astype(jnp.float32)
    gradient = jnp.zeros((3, 2, ATOMS), jnp.float32)
    for offset_x in range(ORDER):
        for offset_y in range(ORDER):
            for offset_z in range(ORDER):
                index_x = (grid_base[0] + offset_x) % KX
                index_y = (grid_base[1] + offset_y) % KY
                index_z = (grid_base[2] + offset_z) % KZ
                sample = potential[:, index_x, index_y, index_z]
                part_x = spline_slope[0, offset_x] * spline[1, offset_y] * spline[2, offset_z]
                part_y = spline[0, offset_x] * spline_slope[1, offset_y] * spline[2, offset_z]
                part_z = spline[0, offset_x] * spline[1, offset_y] * spline_slope[2, offset_z]
                gradient = gradient + jnp.stack([part_x, part_y, part_z])[:, None] * sample[None]
    reciprocal = -((1.0 - weight_b) * charge_a * gradient[:, 0] + weight_b * charge_b * gradient[:, 1])
    packet = jnp.concatenate([positions, charge_a[None], charge_b[None]], axis=0).reshape(5, N_PX, ATOMS_DEV)
    ghost_table = ghost_lists.reshape(2, N_PX, GH_DEV)
    to_right = jnp.take_along_axis(packet, jnp.broadcast_to(ghost_table[0][None], (5, N_PX, GH_DEV)), axis=2)
    to_left = jnp.take_along_axis(packet, jnp.broadcast_to(ghost_table[1][None], (5, N_PX, GH_DEV)), axis=2)
    from_left = jnp.roll(to_right, 1, axis=1)
    from_right = jnp.roll(to_left, -1, axis=1)
    device_ids = jnp.arange(N_PX, dtype=jnp.int32)
    from_left = from_left.at[0].add(-KX * (device_ids == 0).astype(jnp.float32)[:, None])
    from_right = from_right.at[0].add(KX * (device_ids == N_PX - 1).astype(jnp.float32)[:, None])
    candidates = jnp.concatenate([packet, from_left, from_right], axis=2)
    tile_lists = pair_tiles.reshape(N_PX, ATOMS_DEV // TILE, NBR)

    def one_device(inputs):
        return device_pairs(inputs[0], inputs[1], inputs[2], weight_b)
    real_space = lax.map(one_device, (jnp.moveaxis(packet, 1, 0), jnp.moveaxis(candidates, 1, 0), tile_lists))
    real_space = jnp.moveaxis(real_space, 0, 1).reshape(3, ATOMS)
    return reciprocal + real_space
```

```python
import functools
import math
import numpy as np
import jax
import jax.numpy as jnp
from jax import lax
from jax.experimental import pallas as pl
from jax.experimental.pallas import tpu as pltpu
from jax.sharding import PartitionSpec as P

TILE = 128
beta = 0.35
soften_sq = 0.25
VMEM_LIMIT = 60 * 1024 * 1024


def low_part(value):
    return value - value.astype(jnp.bfloat16).astype(jnp.float32)


def three_parts(value):
    first = value.astype(jnp.bfloat16).astype(jnp.float32)
    rest = value - first
    second = rest.astype(jnp.bfloat16).astype(jnp.float32)
    return first, second, rest - second


def dot(left, right, dims=((1,), (0,))):
    return lax.dot_general(left, right, (dims, ((), ())), preferred_element_type=jnp.float32)


def dot3(left, right):
    return dot(left, right) + (dot(low_part(left), right) + dot(left, low_part(right)))


def spline_columns(base_row, weights, length):
    lanes = base_row.shape[1]
    cells = lax.broadcasted_iota(jnp.int32, (length, lanes), 0)
    offset = (cells - base_row) & (length - 1)
    results = []
    for table in weights:
        value = jnp.zeros((length, lanes), jnp.float32)
        for step in reversed(range(len(table))):
            value = jnp.where(offset == step, table[step], value)
        results.append(value)
    return results


def dft_tables(length):
    index = np.arange(length)
    angle = 2.0 * np.pi * ((index[:, None] * index[None, :]) % length) / length
    cosine, sine = np.cos(angle), np.sin(angle)
    forward = np.block([[cosine, -sine], [sine, cosine]]).astype(np.float32)
    return forward, np.ascontiguousarray(forward.T)


def spread_kernel(chunk, charges_ref, base_ref, spline_ref, packet_ref, ghost_ref,
                  *out_refs):
    layer_refs, left_ref, right_ref, total = out_refs[:-3], out_refs[-3], out_refs[-2], out_refs[-1]
    order = len(layer_refs)
    full_y, full_z = layer_refs[0].shape[1:]
    atoms = charges_ref.shape[1]
    ghosts = ghost_ref.shape[1]
    total[...] = jnp.zeros_like(total)

    def body(step, carry):
        at = pl.ds(pl.multiple_of(step * chunk, chunk), chunk)
        base = base_ref[:, at]
        weights = spline_ref[:, :, at]
        charges = charges_ref[:, at]
        rows_y, = spline_columns(base[1:2], [[weights[1, o][None] for o in range(order)]], full_y)
        rows_z, = spline_columns(base[2:3], [[weights[2, o][None] for o in range(order)]], full_z)
        both_z = jnp.concatenate([rows_z, low_part(rows_z)], axis=0)
        for state in range(2):
            for layer in range(order):
                row = charges[state:state + 1] * weights[0, layer][None]
                lifted = row * rows_y
                wide = dot(lifted, both_z, ((1,), (1,)))
                part = wide[:, :full_z] + wide[:, full_z:]
                part = part + dot(low_part(lifted), rows_z, ((1,), (1,)))
                at_rows = pl.ds((state * order + layer) * full_y, full_y)
                total[at_rows, :] += part
        return carry

    lax.fori_loop(0, atoms // chunk, body, 0)
    for state in range(2):
        for layer in range(order):
            first = (state * order + layer) * full_y
            layer_refs[layer][state] = total[first:first + full_y, :]

    def pick(step, carry):
        at = pl.ds(pl.multiple_of(step * chunk, chunk), chunk)
        rows = packet_ref[:, at]
        parts = jnp.concatenate(three_parts(rows), axis=0)
        ids = lax.broadcasted_iota(jnp.int32, (chunk, ghosts), 0) + step * chunk
        results = []
        for side in range(2):
            chosen = jnp.where(ids == ghost_ref[side:side + 1, :], 1.0, 0.0)
            results.append(carry[side] + dot(parts, chosen))
        return tuple(results)

    height = packet_ref.shape[0]
    start = jnp.zeros((3 * height, ghosts), jnp.float32)
    sides = lax.fori_loop(0, atoms // chunk, pick, (start, start))
    for ref, value in zip((left_ref, right_ref), sides):
        ref[...] = value[:height] + value[height:2 * height] + value[2 * height:]


def forward_kernel(own_ref, *refs):
    arrived, (table_ref, tablet_ref, out_ref) = refs[:-3], refs[-3:]
    full_y, full_z = own_ref.shape[1:]
    value = own_ref[...]
    for ref in arrived:
        value = value + ref[...]
    rows = jnp.concatenate([value[0], value[1]], axis=1)
    rows = dot3(rows, table_ref[...])
    columns = jnp.concatenate([rows[:, :full_z], rows[:, full_z:]], axis=0)
    columns = dot3(tablet_ref[...], columns)
    out_ref[0] = columns[:full_y]
    out_ref[1] = columns[full_y:]


def middle_kernel(scale, in_ref, influence_ref, table_ref, tablet_ref, out_ref):
    length = in_ref.shape[1]
    columns = jnp.concatenate([in_ref[0], in_ref[1]], axis=0)
    columns = dot3(tablet_ref[...], columns)
    gain = influence_ref[...] * scale
    columns = columns * jnp.concatenate([gain, gain], axis=0)
    columns = dot3(table_ref[...], columns)
    out_ref[0] = columns[:length]
    out_ref[1] = columns[length:]


def inverse_kernel(in_ref, table_ref, tablet_ref, out_ref):
    full_y, full_z = in_ref.shape[1:]
    columns = jnp.concatenate([in_ref[0], in_ref[1]], axis=0)
    columns = dot3(table_ref[...], columns)
    rows = jnp.concatenate([columns[:full_y], columns[full_y:]], axis=1)
    rows = dot3(rows, tablet_ref[...])
    out_ref[0] = rows[:, :full_z]
    out_ref[1] = rows[:, full_z:]


def sum_tiles(value):
    rows, lanes = value.shape
    return jnp.sum(value.reshape(rows // 8, 8, lanes), axis=0)


def gather_kernel(chunk, order, coupling_ref, charges_ref, base_ref, spline_ref, slope_ref,
                  real_ref, *refs):
    plane_refs, (out_ref, planes) = refs[:-2], refs[-2:]
    full_y, full_z = plane_refs[0].shape[1:]
    atoms = charges_ref.shape[1]
    weight_b = coupling_ref[0]
    for state in range(2):
        for layer in range(order):
            first = (state * order + layer) * full_y
            value = plane_refs[layer][state]
            planes[first:first + full_y, :full_z] = value
            planes[first:first + full_y, full_z:] = low_part(value)

    def body(step, carry):
        at = pl.ds(pl.multiple_of(step * chunk, chunk), chunk)
        base = base_ref[:, at]
        weights = spline_ref[:, :, at]
        slopes = slope_ref[:, :, at]
        charges = charges_ref[:, at]

        def both(axis):
            return spline_columns(
                base[axis:axis + 1],
                [[table[axis, o][None] for o in range(order)] for table in (weights, slopes)],
                full_y)

        rows_y, slope_y = both(1)
        rows_z, slope_z = both(2)
        stacked_z = jnp.concatenate([rows_z, slope_z], axis=1)
        twice_z = jnp.concatenate([stacked_z, stacked_z], axis=0)
        low_z = low_part(stacked_z)
        sums = [jnp.zeros((8, chunk), jnp.float32) for _ in range(3)]
        for state in range(2):
            mix = -(1.0 - weight_b) if state == 0 else -weight_b
            scale = charges[state:state + 1] * mix
            for layer in range(order):
                rows = planes[pl.ds((state * order + layer) * full_y, full_y), :]
                sampled = dot(rows, twice_z) + dot(rows[:, :full_z], low_z)
                plain, sloped = sampled[:, :chunk], sampled[:, chunk:]
                plain_x = scale * weights[0, layer][None]
                slope_x = scale * slopes[0, layer][None]
                sums[0] = sums[0] + slope_x * sum_tiles(plain * rows_y)
                sums[1] = sums[1] + plain_x * sum_tiles(plain * slope_y)
                sums[2] = sums[2] + plain_x * sum_tiles(sloped * rows_y)
        for axis in range(3):
            out_ref[axis:axis + 1, at] = (
                jnp.sum(sums[axis], axis=0, keepdims=True) + real_ref[axis:axis + 1, at])
        return carry

    lax.fori_loop(0, atoms // chunk, body, 0)


def pair_features(scaled, home):
    first, second, third = three_parts(scaled)
    square = jnp.sum(scaled * scaled, axis=0, keepdims=True)
    ones = jnp.ones_like(square)
    if home:
        square = three_parts(square + soften_sq * beta * beta)
        rows = [first, first, second, second, first, third, *square, ones, ones, ones]
    else:
        square = three_parts(square)
        rows = [-2.0 * part for part in (first, second, first, second, third, first)]
        rows = rows + [ones, ones, ones, *square]
    rows.append(jnp.zeros((8, scaled.shape[1]), jnp.float32))
    return jnp.concatenate(rows, axis=0)


def pair_place(rows, shift, first_tile, near_table, source_table, home_table):
    local = jnp.concatenate([rows[0:1] + (shift - 0.5), rows[1:3] - 4.0], axis=0)
    scaled = local * beta
    q_a, q_b = rows[3:4], rows[4:5]
    source = jnp.concatenate([q_a, q_a * local, q_b, q_b * local], axis=0)
    source = jnp.concatenate([*three_parts(source), jnp.zeros_like(source)], axis=0)
    near = pair_features(scaled, False)
    near = jnp.concatenate([near, near, jnp.zeros((64, rows.shape[1]), jnp.float32)], axis=0)
    home = None if home_table is None else pair_features(scaled, True)
    for tile in range(rows.shape[1] // TILE):
        part = slice(tile * TILE, (tile + 1) * TILE)
        near_table[first_tile + tile] = near[:, part].T
        source_table[first_tile + tile] = source[:, part]
        if home is not None:
            home_table[first_tile + tile] = home[:, part]


def pair_own(slab_start, packet_ref, near_table, source_table, home_table, width=512):
    def own(step, carry):
        at = pl.ds(pl.multiple_of(step * width, width), width)
        pair_place(packet_ref[:, at], -slab_start, step * (width // TILE), near_table, source_table,
                   home_table)
        return carry

    lax.fori_loop(0, packet_ref.shape[1] // width, own, 0)


def pair_ghosts(slab_start, length, left_ref, right_ref, is_first, is_last, tiles, near_table,
                source_table):
    extra = left_ref.shape[1] // TILE
    pair_place(left_ref[...], -slab_start - is_first * length, tiles, near_table, source_table, None)
    pair_place(right_ref[...], -slab_start + is_last * length, tiles + extra, near_table,
               source_table, None)


def pair_tile(tile, packet_ref, slab_start, weight_b, lists_ref, near_table, source_table, home_table,
              out_ref):
    slots = lists_ref.shape[1]
    at = pl.ds(pl.multiple_of(tile * TILE, TILE), TILE)
    home = home_table[tile]
    blank = jnp.zeros_like(home)
    rest = jnp.zeros((TILE - 2 * home.shape[0], 2 * TILE), jnp.float32)
    wide_home = jnp.concatenate(
        [jnp.concatenate([home, blank], axis=1), jnp.concatenate([blank, home], axis=1), rest], axis=0)
    lane = lax.broadcasted_iota(jnp.int32, (TILE, TILE), 1)
    total = jnp.zeros((32, 2 * TILE), jnp.float32)
    for slot in range(0, slots, 2):
        one, two = lists_ref[tile, slot], lists_ref[tile, slot + 1]
        near = jnp.where(lane < 32, near_table[one], near_table[two])
        source = jnp.concatenate([source_table[one], source_table[two]], axis=1)
        square = dot(near, wide_home)
        inverse = lax.rsqrt(square)
        tail = (1.0 - lax.erf(square * inverse)) * inverse
        gauss = jnp.exp2(square * (-1.0 / math.log(2.0))) * (2.0 / math.sqrt(math.pi))
        radial = (tail + gauss) * (inverse * inverse)
        low = low_part(radial)
        both = jnp.concatenate(
            [jnp.concatenate([radial[:, :TILE], low[:, :TILE]], axis=1),
             jnp.concatenate([radial[:, TILE:], low[:, TILE:]], axis=1)], axis=0)
        total = total + dot(source, both)
    sums = total[:, :TILE] + total[:, TILE:]
    sums = sums[0:8] + sums[8:16] + sums[16:24]
    rows = packet_ref[:, at]
    local = jnp.concatenate([rows[0:1] - (slab_start + 0.5), rows[1:3] - 4.0], axis=0)
    scale = beta ** 3
    part_a = local * sums[0:1] - sums[1:4]
    part_b = local * sums[4:5] - sums[5:8]
    out_ref[:, at] = (
        ((1.0 - weight_b) * scale) * rows[3:4] * part_a + (weight_b * scale) * rows[4:5] * part_b)


def pair_kernel(length, coupling_ref, place_ref, lists_ref, packet_ref, left_ref, right_ref, out_ref,
                near_table, source_table, home_table):
    slab_start = place_ref[0]
    tiles = lists_ref.shape[0]
    pair_own(slab_start, packet_ref, near_table, source_table, home_table)
    pair_ghosts(slab_start, length, left_ref, right_ref, place_ref[1], place_ref[2], tiles,
                near_table, source_table)

    def body(tile, carry):
        pair_tile(tile, packet_ref, slab_start, coupling_ref[0], lists_ref, near_table, source_table,
                  home_table, out_ref)
        return carry

    lax.fori_loop(0, tiles, body, 0)


VM = pl.BlockSpec(memory_space=pltpu.VMEM)
SM = pl.BlockSpec(memory_space=pltpu.SMEM)
params = pltpu.CompilerParams(vmem_limit_bytes=VMEM_LIMIT)


def f32(*shape):
    return jax.ShapeDtypeStruct(shape, jnp.float32)


def run_spread(charges, grid_base, spline, packet, ghosts, full_y, full_z, chunk=512):
    order = spline.shape[1]
    gh = ghosts.shape[1]
    return pl.pallas_call(
        functools.partial(spread_kernel, chunk),
        out_shape=[f32(2, full_y, full_z)] * order + [f32(8, gh)] * 2,
        in_specs=[VM] * 5, out_specs=[VM] * (order + 2),
        scratch_shapes=[pltpu.VMEM((2 * order * full_y, full_z), jnp.float32)],
        compiler_params=params,
    )(charges, grid_base, spline, packet, ghosts)


def run_gather(coupling, charges, grid_base, spline, slope, real, planes, chunk=128):
    order = spline.shape[1]
    full_y, full_z = planes[0].shape[1:]
    return pl.pallas_call(
        functools.partial(gather_kernel, chunk, order),
        out_shape=f32(3, charges.shape[1]),
        in_specs=[SM] + [VM] * (5 + order), out_specs=VM,
        scratch_shapes=[pltpu.VMEM((2 * order * full_y, 2 * full_z), jnp.float32)],
        compiler_params=params,
    )(coupling, charges, grid_base, spline, slope, real, *planes)


def run_pairs(length, coupling, place, lists, packet, left, right):
    tiles = packet.shape[1] // TILE
    every = tiles + 2 * (left.shape[1] // TILE)
    return pl.pallas_call(
        functools.partial(pair_kernel, length),
        out_shape=f32(3, packet.shape[1]),
        in_specs=[SM] * 3 + [VM] * 3, out_specs=VM,
        scratch_shapes=[pltpu.VMEM((every, TILE, TILE), jnp.float32),
                        pltpu.VMEM((every, 32, TILE), jnp.float32),
                        pltpu.VMEM((tiles, 32, TILE), jnp.float32)],
        compiler_params=params,
    )(coupling, place, lists, packet, left, right)


def run_plain(kernel, out_shape, *operands):
    return pl.pallas_call(
        kernel, out_shape=out_shape, in_specs=[VM] * len(operands), out_specs=VM,
        compiler_params=params)(*operands)


def from_behind(value, axis, steps):
    count = lax.axis_size(axis)
    pairs = [(source, (source + steps) % count) for source in range(count)]
    return lax.ppermute(value, axis, pairs)


def per_device(charge_a, charge_b, coupling, positions, grid_base, spline, spline_slope, influence,
               pair_tiles, ghost_lists):
    group_size = lax.axis_size("px")
    me_index = lax.axis_index("px")
    full_x, slab_y, full_z = influence.shape
    full_y = slab_y * group_size
    order = spline.shape[1]
    charges = jnp.stack([charge_a, charge_b])
    packet = jnp.concatenate(
        [positions, charges, jnp.zeros((3, charges.shape[1]), jnp.float32)], axis=0)
    *layers, to_right, to_left = run_spread(
        charges, grid_base, spline, packet, ghost_lists, full_y, full_z)
    arrived = [from_behind(layers[d], "px", d) for d in range(1, order)]
    from_left = from_behind(to_right, "px", 1)
    from_right = from_behind(to_left, "px", -1)
    table, tablet = (jnp.asarray(value) for value in dft_tables(full_x))
    plane_shape = f32(2, full_y, full_z)
    plane = run_plain(forward_kernel, plane_shape, layers[0], *arrived, table, tablet)
    columns = lax.all_to_all(
        plane[:, None], "px", split_axis=2, concat_axis=1, tiled=True)[:, :, 0]
    columns = run_plain(
        functools.partial(middle_kernel, 1.0 / (full_x * full_y * full_z)), f32(2, full_x, full_z),
        columns, influence[:, 0], table, tablet)
    plane = lax.all_to_all(
        columns[:, :, None], "px", split_axis=1, concat_axis=2, tiled=True)[:, 0]
    plane = run_plain(inverse_kernel, plane_shape, plane, table, tablet)
    planes = [plane] + [from_behind(plane, "px", -d) for d in range(1, order)]
    place = jnp.stack([me_index, me_index == 0, me_index == group_size - 1]).astype(jnp.float32)
    real_space = run_pairs(
        float(full_x), coupling, place, pair_tiles, packet, from_left, from_right)
    return run_gather(coupling, charges, grid_base, spline, spline_slope, real_space, planes)


def solution(mesh):
    placed = (
        P(("win", "px")),
        P(("win", "px")),
        P("win"),
        P(None, ("win", "px")),
        P(None, ("win", "px")),
        P(None, None, ("win", "px")),
        P(None, None, ("win", "px")),
        P(None, "px", None),
        P(("win", "px"), None),
        P(None, ("win", "px")),
    )
    return jax.shard_map(
        per_device, mesh=mesh, in_specs=placed, out_specs=P(None, ("win", "px")), check_vma=False
    )
```

```python
import functools
import math
import numpy as np
import jax
import jax.numpy as jnp
from jax import lax
from jax.experimental import pallas as pl
from jax.experimental.pallas import tpu as pltpu
from jax.sharding import PartitionSpec as P

TILE = 128
beta = 0.35
soften_sq = 0.25
VMEM_LIMIT = 60 * 1024 * 1024


def low_part(value):
    return value - value.astype(jnp.bfloat16).astype(jnp.float32)


def three_parts(value):
    first = value.astype(jnp.bfloat16).astype(jnp.float32)
    rest = value - first
    second = rest.astype(jnp.bfloat16).astype(jnp.float32)
    return first, second, rest - second


def dot(left, right, dims=((1,), (0,))):
    return lax.dot_general(left, right, (dims, ((), ())), preferred_element_type=jnp.float32)


def dot3(left, right):
    return dot(left, right) + (dot(low_part(left), right) + dot(left, low_part(right)))


def spline_columns(base_row, weights, length):
    lanes = base_row.shape[1]
    cells = lax.broadcasted_iota(jnp.int32, (length, lanes), 0)
    offset = (cells - base_row) & (length - 1)
    results = []
    for table in weights:
        value = jnp.zeros((length, lanes), jnp.float32)
        for step in reversed(range(len(table))):
            value = jnp.where(offset == step, table[step], value)
        results.append(value)
    return results


def dft_tables(length):
    index = np.arange(length)
    angle = 2.0 * np.pi * ((index[:, None] * index[None, :]) % length) / length
    cosine, sine = np.cos(angle), np.sin(angle)
    forward = np.block([[cosine, -sine], [sine, cosine]]).astype(np.float32)
    return forward, np.ascontiguousarray(forward.T)


def sum_tiles(value):
    rows, lanes = value.shape
    return jnp.sum(value.reshape(rows // 8, 8, lanes), axis=0)


def gather_kernel(chunk, order, coupling_ref, charges_ref, base_ref, spline_ref, slope_ref,
                  real_ref, plane_ref, out_ref, planes):
    full_y, full_z = plane_ref.shape[2:]
    atoms = charges_ref.shape[1]
    weight_b = coupling_ref[0]
    for state in range(2):
        for layer in range(order):
            first = (state * order + layer) * full_y
            value = plane_ref[layer, state]
            planes[first:first + full_y, :full_z] = value
            planes[first:first + full_y, full_z:] = low_part(value)

    def body(step, carry):
        at = pl.ds(pl.multiple_of(step * chunk, chunk), chunk)
        base = base_ref[:, at]
        weights = spline_ref[:, :, at]
        slopes = slope_ref[:, :, at]
        charges = charges_ref[:, at]

        def both(axis):
            return spline_columns(
                base[axis:axis + 1],
                [[table[axis, o][None] for o in range(order)] for table in (weights, slopes)],
                full_y)

        rows_y, slope_y = both(1)
        rows_z, slope_z = both(2)
        stacked_z = jnp.concatenate([rows_z, slope_z], axis=1)
        twice_z = jnp.concatenate([stacked_z, stacked_z], axis=0)
        low_z = low_part(stacked_z)
        sums = [jnp.zeros((8, chunk), jnp.float32) for _ in range(3)]
        for state in range(2):
            mix = -(1.0 - weight_b) if state == 0 else -weight_b
            scale = charges[state:state + 1] * mix
            for layer in range(order):
                rows = planes[pl.ds((state * order + layer) * full_y, full_y), :]
                sampled = dot(rows, twice_z) + dot(rows[:, :full_z], low_z)
                plain, sloped = sampled[:, :chunk], sampled[:, chunk:]
                plain_x = scale * weights[0, layer][None]
                slope_x = scale * slopes[0, layer][None]
                sums[0] = sums[0] + slope_x * sum_tiles(plain * rows_y)
                sums[1] = sums[1] + plain_x * sum_tiles(plain * slope_y)
                sums[2] = sums[2] + plain_x * sum_tiles(sloped * rows_y)
        for axis in range(3):
            out_ref[axis:axis + 1, at] = (
                jnp.sum(sums[axis], axis=0, keepdims=True) + real_ref[axis:axis + 1, at])
        return carry

    lax.fori_loop(0, atoms // chunk, body, 0)


def pair_features(scaled, home):
    first, second, third = three_parts(scaled)
    square = jnp.sum(scaled * scaled, axis=0, keepdims=True)
    ones = jnp.ones_like(square)
    if home:
        square = three_parts(square + soften_sq * beta * beta)
        rows = [first, first, second, second, first, third, *square, ones, ones, ones]
    else:
        square = three_parts(square)
        rows = [-2.0 * part for part in (first, second, first, second, third, first)]
        rows = rows + [ones, ones, ones, *square]
    rows.append(jnp.zeros((8, scaled.shape[1]), jnp.float32))
    return jnp.concatenate(rows, axis=0)


def pair_place(rows, shift, first_tile, near_table, source_table, home_table):
    local = jnp.concatenate([rows[0:1] + (shift - 0.5), rows[1:3] - 4.0], axis=0)
    scaled = local * beta
    q_a, q_b = rows[3:4], rows[4:5]
    source = jnp.concatenate([q_a, q_a * local, q_b, q_b * local], axis=0)
    source = jnp.concatenate([*three_parts(source), jnp.zeros_like(source)], axis=0)
    near = pair_features(scaled, False)
    near = jnp.concatenate([near, near, jnp.zeros((64, rows.shape[1]), jnp.float32)], axis=0)
    home = None if home_table is None else pair_features(scaled, True)
    for tile in range(rows.shape[1] // TILE):
        part = slice(tile * TILE, (tile + 1) * TILE)
        near_table[first_tile + tile] = near[:, part].T
        source_table[first_tile + tile] = source[:, part]
        if home is not None:
            home_table[first_tile + tile] = home[:, part]


def pair_own(slab_start, packet_ref, near_table, source_table, home_table, width=512):
    def own(step, carry):
        at = pl.ds(pl.multiple_of(step * width, width), width)
        pair_place(packet_ref[:, at], -slab_start, step * (width // TILE), near_table, source_table,
                   home_table)
        return carry

    lax.fori_loop(0, packet_ref.shape[1] // width, own, 0)


def pair_ghosts(slab_start, length, left_ref, right_ref, is_first, is_last, tiles, near_table,
                source_table):
    extra = left_ref.shape[1] // TILE
    pair_place(left_ref[...], -slab_start - is_first * length, tiles, near_table, source_table, None)
    pair_place(right_ref[...], -slab_start + is_last * length, tiles + extra, near_table,
               source_table, None)


def pair_tile(tile, packet_ref, slab_start, weight_b, lists_ref, near_table, source_table, home_table,
              out_ref):
    slots = lists_ref.shape[1]
    at = pl.ds(pl.multiple_of(tile * TILE, TILE), TILE)
    home = home_table[tile]
    blank = jnp.zeros_like(home)
    rest = jnp.zeros((TILE - 2 * home.shape[0], 2 * TILE), jnp.float32)
    wide_home = jnp.concatenate(
        [jnp.concatenate([home, blank], axis=1), jnp.concatenate([blank, home], axis=1), rest], axis=0)
    lane = lax.broadcasted_iota(jnp.int32, (TILE, TILE), 1)
    total = jnp.zeros((32, 2 * TILE), jnp.float32)
    for slot in range(0, slots, 2):
        one, two = lists_ref[tile, slot], lists_ref[tile, slot + 1]
        near = jnp.where(lane < 32, near_table[one], near_table[two])
        source = jnp.concatenate([source_table[one], source_table[two]], axis=1)
        square = dot(near, wide_home)
        inverse = lax.rsqrt(square)
        tail = (1.0 - lax.erf(square * inverse)) * inverse
        gauss = jnp.exp2(square * (-1.0 / math.log(2.0))) * (2.0 / math.sqrt(math.pi))
        radial = (tail + gauss) * (inverse * inverse)
        low = low_part(radial)
        both = jnp.concatenate(
            [jnp.concatenate([radial[:, :TILE], low[:, :TILE]], axis=1),
             jnp.concatenate([radial[:, TILE:], low[:, TILE:]], axis=1)], axis=0)
        total = total + dot(source, both)
    sums = total[:, :TILE] + total[:, TILE:]
    sums = sums[0:8] + sums[8:16] + sums[16:24]
    rows = packet_ref[:, at]
    local = jnp.concatenate([rows[0:1] - (slab_start + 0.5), rows[1:3] - 4.0], axis=0)
    scale = beta ** 3
    part_a = local * sums[0:1] - sums[1:4]
    part_b = local * sums[4:5] - sums[5:8]
    out_ref[:, at] = (
        ((1.0 - weight_b) * scale) * rows[3:4] * part_a + (weight_b * scale) * rows[4:5] * part_b)


VM = pl.BlockSpec(memory_space=pltpu.VMEM)
SM = pl.BlockSpec(memory_space=pltpu.SMEM)
params = pltpu.CompilerParams(vmem_limit_bytes=VMEM_LIMIT)


def f32(*shape):
    return jax.ShapeDtypeStruct(shape, jnp.float32)


def run_gather(coupling, charges, grid_base, spline, slope, real, planes, chunk=128):
    order = spline.shape[1]
    full_y, full_z = planes.shape[2:]
    return pl.pallas_call(
        functools.partial(gather_kernel, chunk, order),
        out_shape=f32(3, charges.shape[1]),
        in_specs=[SM] + [VM] * 6, out_specs=VM,
        scratch_shapes=[pltpu.VMEM((2 * order * full_y, 2 * full_z), jnp.float32)],
        compiler_params=params,
    )(coupling, charges, grid_base, spline, slope, real, planes)


MESH = pl.DeviceIdType.MESH


def spread_atoms(chunk, charges_ref, base_ref, spline_ref, spread_out):
    order, _, full_y, full_z = spread_out.shape
    spread_out[...] = jnp.zeros_like(spread_out)

    def body(step, carry):
        at = pl.ds(pl.multiple_of(step * chunk, chunk), chunk)
        base = base_ref[:, at]
        weights = spline_ref[:, :, at]
        charges = charges_ref[:, at]
        rows_y, = spline_columns(base[1:2], [[weights[1, o][None] for o in range(order)]], full_y)
        rows_z, = spline_columns(base[2:3], [[weights[2, o][None] for o in range(order)]], full_z)
        both_z = jnp.concatenate([rows_z, low_part(rows_z)], axis=0)
        for state in range(2):
            for layer in range(order):
                row = charges[state:state + 1] * weights[0, layer][None]
                lifted = row * rows_y
                wide = dot(lifted, both_z, ((1,), (1,)))
                part = wide[:, :full_z] + wide[:, full_z:]
                part = part + dot(low_part(lifted), rows_z, ((1,), (1,)))
                spread_out[layer, state] += part
        return carry

    lax.fori_loop(0, charges_ref.shape[1] // chunk, body, 0)


def pick_ghosts(chunk, packet_ref, ghost_ref, ghost_out):
    height, atoms = packet_ref.shape
    ghosts = ghost_ref.shape[1]

    def pick(step, carry):
        at = pl.ds(pl.multiple_of(step * chunk, chunk), chunk)
        parts = jnp.concatenate(three_parts(packet_ref[:, at]), axis=0)
        ids = lax.broadcasted_iota(jnp.int32, (chunk, ghosts), 0) + step * chunk
        results = []
        for side in range(2):
            chosen = jnp.where(ids == ghost_ref[side:side + 1, :], 1.0, 0.0)
            results.append(carry[side] + dot(parts, chosen))
        return tuple(results)

    start = jnp.zeros((3 * height, ghosts), jnp.float32)
    sides = lax.fori_loop(0, atoms // chunk, pick, (start, start))
    for side, value in enumerate(sides):
        ghost_out[side] = value[:height] + value[height:2 * height] + value[2 * height:]


def step_kernel(group, windows, scale, coupling_ref, lists_ref, charges_ref, base_ref, spline_ref,
                packet_ref, ghost_ref, influence_ref, table_ref, tablet_ref,
                plane_ref, real_ref,
                spread_out, halo_in, ghost_out, ghost_in, there_out, there_in, back_out, back_in,
                plane_in, near_table, source_table, home_table,
                halo_send, halo_recv, ghost_send, ghost_recv, row_send, row_recv, row_own,
                plane_send, plane_recv):
    me = lax.axis_index("px")
    order, _, full_y, full_z = spread_out.shape
    full_x = influence_ref.shape[0]
    tiles = lists_ref.shape[0]
    slab_start = me.astype(jnp.float32)

    def other(steps):
        return {"px": lax.rem(me + (steps + group), group)}

    barrier = pltpu.get_barrier_semaphore()

    def greet(steps, carry):
        pl.semaphore_signal(barrier, inc=1, device_id=other(steps), device_id_type=MESH)
        return carry

    lax.fori_loop(1, group, greet, 0)

    spread_atoms(512, charges_ref, base_ref, spline_ref, spread_out)
    pick_ghosts(512, packet_ref, ghost_ref, ghost_out)

    pl.semaphore_wait(barrier, group - 1)

    halos = [
        pltpu.make_async_remote_copy(
            src_ref=spread_out.at[layer], dst_ref=halo_in.at[layer - 1],
            send_sem=halo_send.at[layer - 1], recv_sem=halo_recv.at[layer - 1],
            device_id=other(layer), device_id_type=MESH)
        for layer in range(1, order)]
    visits = [
        pltpu.make_async_remote_copy(
            src_ref=ghost_out.at[side], dst_ref=ghost_in.at[side],
            send_sem=ghost_send.at[side], recv_sem=ghost_recv.at[side],
            device_id=other(1 - 2 * side), device_id_type=MESH)
        for side in range(2)]
    for copy in halos + visits:
        copy.start()
    pair_own(slab_start, packet_ref, near_table, source_table, home_table)
    for copy in halos + visits:
        copy.wait()

    def swap_rows(out_rows, in_rows, which):
        def row_to(steps):
            return pltpu.make_async_remote_copy(
                src_ref=out_rows.at[lax.rem(me + steps, group)], dst_ref=in_rows.at[me],
                send_sem=row_send.at[which], recv_sem=row_recv.at[which],
                device_id=other(steps), device_id_type=MESH)

        own = pltpu.make_async_copy(out_rows.at[me], in_rows.at[me], row_own.at[which])
        own.start()
        half = group // 2
        row_to(half).start()

        def send(steps, carry):
            row_to(half - steps).start()
            row_to(half + steps).start()
            return carry

        lax.fori_loop(1, half, send, 0)

        def finish():
            own.wait()
            every = pltpu.make_async_remote_copy(
                src_ref=out_rows.at[pl.ds(0, group - 1)], dst_ref=in_rows.at[pl.ds(0, group - 1)],
                send_sem=row_send.at[which], recv_sem=row_recv.at[which],
                device_id=other(half), device_id_type=MESH)
            every.wait()

        return finish

    def pairs(first, last):
        def body(tile, carry):
            pair_tile(tile, packet_ref, slab_start, coupling_ref[0], lists_ref, near_table,
                      source_table, home_table, real_ref)
            return carry

        lax.fori_loop(first, last, body, 0)

    table, tablet = table_ref[...], tablet_ref[...]
    value = spread_out[0]
    for layer in range(order - 1):
        value = value + halo_in[layer]
    rows = dot3(jnp.concatenate([value[0], value[1]], axis=1), table)
    columns = dot3(tablet, jnp.concatenate([rows[:, :full_z], rows[:, full_z:]], axis=0))
    there_out[:, 0, :] = columns[:full_y]
    there_out[:, 1, :] = columns[full_y:]
    finish = swap_rows(there_out, there_in, 0)

    is_first = jnp.where(me == 0, 1.0, 0.0)
    is_last = jnp.where(me == group - 1, 1.0, 0.0)
    pair_ghosts(slab_start, float(full_x), ghost_in.at[0], ghost_in.at[1], is_first, is_last, tiles,
                near_table, source_table)
    pairs(0, windows[0])
    finish()

    columns = dot3(tablet, jnp.concatenate([there_in[:, 0, :], there_in[:, 1, :]], axis=0))
    gain = influence_ref[...] * scale
    columns = dot3(table, columns * jnp.concatenate([gain, gain], axis=0))
    back_out[:, 0, :] = columns[:full_x]
    back_out[:, 1, :] = columns[full_x:]
    finish = swap_rows(back_out, back_in, 1)
    pairs(windows[0], windows[1])
    finish()

    columns = dot3(table, jnp.concatenate([back_in[:, 0, :], back_in[:, 1, :]], axis=0))
    rows = dot3(jnp.concatenate([columns[:full_y], columns[full_y:]], axis=1), tablet)
    plane_in[0, 0] = rows[:, :full_z]
    plane_in[0, 1] = rows[:, full_z:]
    lends = [
        pltpu.make_async_remote_copy(
            src_ref=plane_in.at[0], dst_ref=plane_in.at[layer],
            send_sem=plane_send.at[layer - 1], recv_sem=plane_recv.at[layer - 1],
            device_id=other(-layer), device_id_type=MESH)
        for layer in range(1, order)]
    for copy in lends:
        copy.start()
    pairs(windows[1], tiles)
    for copy in lends:
        copy.wait()
    plane_ref[...] = plane_in[...]


def run_step(group, coupling, lists, charges, grid_base, spline, packet, ghosts, influence):
    order = spline.shape[1]
    full_x, full_z = influence.shape
    full_y = group
    atoms = charges.shape[1]
    tiles = lists.shape[0]
    visitors = ghosts.shape[1]
    every = tiles + 2 * (visitors // TILE)
    plane = (2, full_y, full_z)
    table, tablet = (jnp.asarray(value) for value in dft_tables(full_x))
    windows = (tiles * 3 // 8, tiles * 6 // 8)
    return pl.pallas_call(
        functools.partial(step_kernel, group, windows, 1.0 / (full_x * full_y * full_z)),
        out_shape=[f32(order, *plane), f32(3, atoms)],
        in_specs=[SM] * 2 + [VM] * 8,
        out_specs=[VM] * 2,
        scratch_shapes=[
            pltpu.VMEM((order, *plane), jnp.float32),
            pltpu.VMEM((order - 1, *plane), jnp.float32),
            pltpu.VMEM((2, packet.shape[0], visitors), jnp.float32),
            pltpu.VMEM((2, packet.shape[0], visitors), jnp.float32),
            pltpu.VMEM((group, 2, full_z), jnp.float32),
            pltpu.VMEM((group, 2, full_z), jnp.float32),
            pltpu.VMEM((group, 2, full_z), jnp.float32),
            pltpu.VMEM((group, 2, full_z), jnp.float32),
            pltpu.VMEM((order, *plane), jnp.float32),
            pltpu.VMEM((every, TILE, TILE), jnp.float32),
            pltpu.VMEM((every, 32, TILE), jnp.float32),
            pltpu.VMEM((tiles, 32, TILE), jnp.float32),
            pltpu.SemaphoreType.DMA((order - 1,)),
            pltpu.SemaphoreType.DMA((order - 1,)),
            pltpu.SemaphoreType.DMA((2,)),
            pltpu.SemaphoreType.DMA((2,)),
            pltpu.SemaphoreType.DMA((2,)),
            pltpu.SemaphoreType.DMA((2,)),
            pltpu.SemaphoreType.DMA((2,)),
            pltpu.SemaphoreType.DMA((order - 1,)),
            pltpu.SemaphoreType.DMA((order - 1,)),
        ],
        compiler_params=pltpu.CompilerParams(
            vmem_limit_bytes=VMEM_LIMIT, collective_id=0, has_side_effects=True),
    )(coupling, lists, charges, grid_base, spline, packet, ghosts, influence, table, tablet)


def per_device(charge_a, charge_b, coupling, positions, grid_base, spline, spline_slope, influence,
               pair_tiles, ghost_lists):
    group = lax.axis_size("px")
    charges = jnp.stack([charge_a, charge_b])
    packet = jnp.concatenate(
        [positions, charges, jnp.zeros((3, charges.shape[1]), jnp.float32)], axis=0)
    planes, real_space = run_step(
        group, coupling, pair_tiles, charges, grid_base, spline, packet, ghost_lists, influence[:, 0])
    return run_gather(coupling, charges, grid_base, spline, spline_slope, real_space, planes)


def solution(mesh):
    placed = (
        P(("win", "px")),
        P(("win", "px")),
        P("win"),
        P(None, ("win", "px")),
        P(None, ("win", "px")),
        P(None, None, ("win", "px")),
        P(None, None, ("win", "px")),
        P(None, "px", None),
        P(("win", "px"), None),
        P(None, ("win", "px")),
    )
    return jax.shard_map(
        per_device, mesh=mesh, in_specs=placed, out_specs=P(None, ("win", "px")), check_vma=False
    )
```

```python
import functools
import math
import numpy as np
import jax
import jax.numpy as jnp
from jax import lax
from jax.experimental import pallas as pl
from jax.experimental.pallas import tpu as pltpu
from jax.sharding import PartitionSpec as P

TILE = 128
beta = 0.35
soften_sq = 0.25
VMEM_LIMIT = 60 * 1024 * 1024


def low_part(value):
    return value - value.astype(jnp.bfloat16).astype(jnp.float32)


def three_parts(value):
    first = value.astype(jnp.bfloat16).astype(jnp.float32)
    rest = value - first
    second = rest.astype(jnp.bfloat16).astype(jnp.float32)
    return first, second, rest - second


def dot(left, right, dims=((1,), (0,))):
    return lax.dot_general(left, right, (dims, ((), ())), preferred_element_type=jnp.float32)


def dot3(left, right):
    return dot(left, right) + (dot(low_part(left), right) + dot(left, low_part(right)))


def spline_columns(base_row, weights, length):
    lanes = base_row.shape[1]
    cells = lax.broadcasted_iota(jnp.int32, (length, lanes), 0)
    offset = (cells - base_row) & (length - 1)
    results = []
    for table in weights:
        value = jnp.zeros((length, lanes), jnp.float32)
        for step in reversed(range(len(table))):
            value = jnp.where(offset == step, table[step], value)
        results.append(value)
    return results


def dft_tables(length):
    index = np.arange(length)
    angle = 2.0 * np.pi * ((index[:, None] * index[None, :]) % length) / length
    cosine, sine = np.cos(angle), np.sin(angle)
    forward = np.block([[cosine, -sine], [sine, cosine]]).astype(np.float32)
    return forward, np.ascontiguousarray(forward.T)


def sum_tiles(value):
    rows, lanes = value.shape
    return jnp.sum(value.reshape(rows // 8, 8, lanes), axis=0)


def pair_features(scaled, home):
    first, second, third = three_parts(scaled)
    square = jnp.sum(scaled * scaled, axis=0, keepdims=True)
    ones = jnp.ones_like(square)
    if home:
        square = three_parts(square + soften_sq * beta * beta)
        rows = [first, first, second, second, first, third, *square, ones, ones, ones]
    else:
        square = three_parts(square)
        rows = [-2.0 * part for part in (first, second, first, second, third, first)]
        rows = rows + [ones, ones, ones, *square]
    rows.append(jnp.zeros((8, scaled.shape[1]), jnp.float32))
    return jnp.concatenate(rows, axis=0)


def pair_place(rows, shift, first_tile, near_table, source_table, home_table):
    local = jnp.concatenate([rows[0:1] + (shift - 0.5), rows[1:3] - 4.0], axis=0)
    scaled = local * beta
    q_a, q_b = rows[3:4], rows[4:5]
    source = jnp.concatenate([q_a, q_a * local, q_b, q_b * local], axis=0)
    source = jnp.concatenate([*three_parts(source), jnp.zeros_like(source)], axis=0)
    near = pair_features(scaled, False)
    near = jnp.concatenate([near, near, jnp.zeros((64, rows.shape[1]), jnp.float32)], axis=0)
    home = None if home_table is None else pair_features(scaled, True)
    for tile in range(rows.shape[1] // TILE):
        part = slice(tile * TILE, (tile + 1) * TILE)
        near_table[first_tile + tile] = near[:, part].T
        source_table[first_tile + tile] = source[:, part]
        if home is not None:
            home_table[first_tile + tile] = home[:, part]


def pair_own(slab_start, packet_ref, near_table, source_table, home_table, width=512):
    def own(step, carry):
        at = pl.ds(pl.multiple_of(step * width, width), width)
        pair_place(packet_ref[:, at], -slab_start, step * (width // TILE), near_table, source_table,
                   home_table)
        return carry

    lax.fori_loop(0, packet_ref.shape[1] // width, own, 0)


def pair_ghosts(slab_start, length, left_ref, right_ref, is_first, is_last, tiles, near_table,
                source_table):
    extra = left_ref.shape[1] // TILE
    pair_place(left_ref[...], -slab_start - is_first * length, tiles, near_table, source_table, None)
    pair_place(right_ref[...], -slab_start + is_last * length, tiles + extra, near_table,
               source_table, None)


def pair_tile(tile, packet_ref, slab_start, weight_b, lists_ref, near_table, source_table, home_table,
              out_ref):
    slots = lists_ref.shape[0]
    at = pl.ds(pl.multiple_of(tile * TILE, TILE), TILE)
    home = home_table[tile]
    blank = jnp.zeros_like(home)
    rest = jnp.zeros((TILE - 2 * home.shape[0], 2 * TILE), jnp.float32)
    wide_home = jnp.concatenate(
        [jnp.concatenate([home, blank], axis=1), jnp.concatenate([blank, home], axis=1), rest], axis=0)
    lane = lax.broadcasted_iota(jnp.int32, (TILE, TILE), 1)
    total = jnp.zeros((32, 2 * TILE), jnp.float32)
    for slot in range(0, slots, 2):
        one, two = lists_ref[slot, tile], lists_ref[slot + 1, tile]
        near = jnp.where(lane < 32, near_table[one], near_table[two])
        source = jnp.concatenate([source_table[one], source_table[two]], axis=1)
        square = dot(near, wide_home)
        inverse = lax.rsqrt(square)
        tail = (1.0 - lax.erf(square * inverse)) * inverse
        gauss = jnp.exp2(square * (-1.0 / math.log(2.0))) * (2.0 / math.sqrt(math.pi))
        radial = (tail + gauss) * (inverse * inverse)
        low = low_part(radial)
        both = jnp.concatenate(
            [jnp.concatenate([radial[:, :TILE], low[:, :TILE]], axis=1),
             jnp.concatenate([radial[:, TILE:], low[:, TILE:]], axis=1)], axis=0)
        total = total + dot(source, both)
    sums = total[:, :TILE] + total[:, TILE:]
    sums = sums[0:8] + sums[8:16] + sums[16:24]
    rows = packet_ref[:, at]
    local = jnp.concatenate([rows[0:1] - (slab_start + 0.5), rows[1:3] - 4.0], axis=0)
    scale = beta ** 3
    part_a = local * sums[0:1] - sums[1:4]
    part_b = local * sums[4:5] - sums[5:8]
    out_ref[:, at] = (
        ((1.0 - weight_b) * scale) * rows[3:4] * part_a + (weight_b * scale) * rows[4:5] * part_b)


VM = pl.BlockSpec(memory_space=pltpu.VMEM)
SM = pl.BlockSpec(memory_space=pltpu.SMEM)
params = pltpu.CompilerParams(vmem_limit_bytes=VMEM_LIMIT)


def f32(*shape):
    return jax.ShapeDtypeStruct(shape, jnp.float32)


def spread_atoms(chunk, charge_refs, base_ref, spline_ref, spread_out, grid_sum):
    order, _, full_y, full_z = spread_out.shape
    grid_sum[...] = jnp.zeros_like(grid_sum)

    def body(step, carry):
        at = pl.ds(pl.multiple_of(step * chunk, chunk), chunk)
        base = base_ref[:, at]
        weights = spline_ref[:, :, at]
        rows_y, = spline_columns(base[1:2], [[weights[1, o][None] for o in range(order)]], full_y)
        rows_z, = spline_columns(base[2:3], [[weights[2, o][None] for o in range(order)]], full_z)
        left = jnp.concatenate([ref[:, at] * rows_y for ref in charge_refs], axis=0)
        right = jnp.concatenate([weights[0, layer][None] * rows_z for layer in range(order)], axis=0)
        high = dot(jnp.concatenate([left, low_part(left)], axis=0), right, ((1,), (1,)))
        rest = dot(left, low_part(right), ((1,), (1,)))
        grid_sum[...] += high[:2 * full_y] + high[2 * full_y:] + rest
        return carry

    lax.fori_loop(0, base_ref.shape[1] // chunk, body, 0)
    for state in range(2):
        for layer in range(order):
            spread_out[layer, state] = grid_sum[state * full_y:(state + 1) * full_y,
                                                layer * full_z:(layer + 1) * full_z]


def gather_prepare(chunk, weight_b, charge_refs, base_ref, spline_ref, slope_ref, rows_y_ref,
                   slope_y_ref, wide_ref, low_ref, first, last):
    full_y = rows_y_ref.shape[0]
    order = spline_ref.shape[1]

    def body(step, carry):
        at = pl.ds(pl.multiple_of(step * chunk, chunk), chunk)
        twice = pl.ds(pl.multiple_of(step * 2 * chunk, 2 * chunk), 2 * chunk)
        base = base_ref[:, at]
        weights = spline_ref[:, :, at]
        slopes = slope_ref[:, :, at]

        def both(axis):
            return spline_columns(
                base[axis:axis + 1],
                [[table[axis, o][None] for o in range(order)] for table in (weights, slopes)],
                full_y)

        rows_y_ref[:, at], slope_y_ref[:, at] = both(1)
        stacked_z = jnp.concatenate(both(2), axis=1)
        scales = [(weight_b - 1.0) * charge_refs[0][:, at], -weight_b * charge_refs[1][:, at]]
        wide = jnp.concatenate(
            [jnp.concatenate([scale, scale], axis=1) * stacked_z for scale in scales], axis=0)
        wide_ref[:, twice] = wide
        low_ref[:, twice] = low_part(wide)
        return carry

    lax.fori_loop(first, last, body, 0)


def gather_atoms(chunk, spline_ref, slope_ref, plane_ref, rows_y_ref, slope_y_ref, wide_ref, low_ref,
                 out_ref, planes):
    order, _, full_y, full_z = plane_ref.shape
    height = order * full_y
    for state in range(2):
        for layer in range(order):
            value = plane_ref[layer, state]
            lanes = slice(state * full_z, (state + 1) * full_z)
            planes[layer * full_y:(layer + 1) * full_y, lanes] = value
            planes[height + layer * full_y:height + (layer + 1) * full_y, lanes] = low_part(value)

    def body(step, carry):
        at = pl.ds(pl.multiple_of(step * chunk, chunk), chunk)
        twice = pl.ds(pl.multiple_of(step * 2 * chunk, 2 * chunk), 2 * chunk)
        weights = spline_ref[0, :, at]
        slopes = slope_ref[0, :, at]
        rows_y, slope_y = rows_y_ref[:, at], slope_y_ref[:, at]
        high = dot(planes[...], wide_ref[:, twice])
        rest = dot(planes[:height, :], low_ref[:, twice])
        sums = [jnp.zeros((8, chunk), jnp.float32) for _ in range(3)]
        for layer in range(order):
            part = slice(layer * full_y, (layer + 1) * full_y)
            again = slice(height + layer * full_y, height + (layer + 1) * full_y)
            sampled = high[part] + high[again] + rest[part]
            plain, sloped = sampled[:, :chunk], sampled[:, chunk:]
            plain_x, slope_x = weights[layer:layer + 1], slopes[layer:layer + 1]
            sums[0] = sums[0] + slope_x * sum_tiles(plain * rows_y)
            sums[1] = sums[1] + plain_x * sum_tiles(plain * slope_y)
            sums[2] = sums[2] + plain_x * sum_tiles(sloped * rows_y)
        for axis in range(3):
            out_ref[axis:axis + 1, at] = jnp.sum(sums[axis], axis=0, keepdims=True)
        return carry

    lax.fori_loop(0, spline_ref.shape[2] // chunk, body, 0)

MESH = pl.DeviceIdType.MESH
ATOMS_AT_ONCE = 512


def each(first, last, body, width):
    head = (last - first) % width
    for step in range(head):
        body(first + step)

    def block(index, carry):
        for step in range(width):
            body(first + head + index * width + step)
        return carry

    lax.fori_loop(0, (last - first - head) // width, block, 0)


def pick_ghosts(chunk, packet_ref, ghost_ref, ghost_out):
    height, atoms = packet_ref.shape
    ghosts = ghost_ref.shape[1]

    def pick(step, carry):
        at = pl.ds(pl.multiple_of(step * chunk, chunk), chunk)
        parts = jnp.concatenate(three_parts(packet_ref[:, at]), axis=0)
        ids = lax.broadcasted_iota(jnp.int32, (chunk, ghosts), 0) + step * chunk
        results = []
        for side in range(2):
            chosen = jnp.where(ids == ghost_ref[side:side + 1, :], 1.0, 0.0)
            results.append(carry[side] + dot(parts, chosen))
        return tuple(results)

    start = jnp.zeros((3 * height, ghosts), jnp.float32)
    sides = lax.fori_loop(0, atoms // chunk, pick, (start, start))
    for side, value in enumerate(sides):
        ghost_out[side] = value[:height] + value[height:2 * height] + value[2 * height:]


def step_kernel(group, windows, scale, coupling_ref, lists_ref, *refs):
    inputs, (out_ref, real_ref), held, refs = refs[:10], refs[10:12], refs[12:22], refs[22:]
    (charge_a_ref, charge_b_ref, base_ref, spline_ref, position_ref, ghost_ref, slope_ref, table_ref,
     tablet_ref, influence_ref) = held
    (input_sem, rows_y, slope_y, wide_z, low_z, packet_ref, grid_sum, planes, spread_out, near_in, far_out, far_in, ghost_out, ghost_in, there_out, there_in, back_out, back_in,
     plane_in, near_table, source_table, home_table,
     near_send, near_recv, far_send, far_recv, ghost_send, ghost_recv, row_send, row_recv, row_own,
     plane_send, plane_recv) = refs
    loads = [pltpu.make_async_copy(src, dst, input_sem.at[index])
             for index, (src, dst) in enumerate(zip(inputs, held))]
    for copy in loads:
        copy.start()
    me = lax.axis_index("px")
    order, _, full_y, full_z = spread_out.shape
    full_x = influence_ref.shape[0]
    tiles = lists_ref.shape[1]
    slab_start = me.astype(jnp.float32)

    def other(steps):
        return {"px": lax.rem(me + (steps + group), group)}

    barrier = pltpu.get_barrier_semaphore()

    def greet(steps):
        pl.semaphore_signal(barrier, inc=1, device_id=other(steps), device_id_type=MESH)

    with jax.named_scope("greet"):
        each(1, group, greet, 14)

    charge_refs = (charge_a_ref, charge_b_ref)
    for copy in loads[:4]:
        copy.wait()
    with jax.named_scope("spread"):
        spread_atoms(2048, charge_refs, base_ref, spline_ref, spread_out, grid_sum)

    with jax.named_scope("barrier_wait"):
        pl.semaphore_wait(barrier, group - 1)

    odd = lax.rem(me, 2)
    partner = other(1 - 2 * odd)

    def carry_to(device, src, dst, sends, recvs, at):
        return pltpu.make_async_remote_copy(
            src_ref=src, dst_ref=dst, send_sem=sends.at[at], recv_sem=recvs.at[at],
            device_id=device, device_id_type=MESH)

    third = [carry_to(other(1), spread_out.at[3, s], near_in.at[1, s], near_send, near_recv, 2 + s)
             for s in range(2)]
    first = [carry_to(partner, spread_out.at[1, s], near_in.at[0, s], near_send, near_recv, s)
             for s in range(2)]
    far = [carry_to(other(2), far_out.at[s], far_in.at[s], far_send, far_recv, s) for s in range(2)]
    visits = [carry_to(other(1 - 2 * side), ghost_out.at[side], ghost_in.at[side], ghost_send,
                       ghost_recv, side) for side in range(2)]
    for copy in third + first:
        copy.start()
    for copy in loads[4:]:
        copy.wait()
    with jax.named_scope("pick"):
        packet_ref[0:3, :] = position_ref[...]
        packet_ref[3:4, :] = charge_a_ref[...]
        packet_ref[4:5, :] = charge_b_ref[...]
        packet_ref[5:8, :] = jnp.zeros_like(position_ref)
        pick_ghosts(512, packet_ref, ghost_ref, ghost_out)
    prepare = functools.partial(gather_prepare, ATOMS_AT_ONCE, coupling_ref[0], charge_refs, base_ref,
                                spline_ref, slope_ref, rows_y, slope_y, wide_z, low_z)
    with jax.named_scope("prepare_a"):
        prepare(0, 2)
    with jax.named_scope("wait_near"):
        for s in range(2):
            first[s].wait()
            third[s].wait()
            far_out[s] = spread_out[2, s] + near_in[1, s] + jnp.where(odd == 0, near_in[0, s], 0.0)
            far[s].start()
    for copy in visits:
        copy.start()
    with jax.named_scope("pair_own"):
        pair_own(slab_start, packet_ref, near_table, source_table, home_table)
    with jax.named_scope("prepare_b"):
        prepare(2, 5)
    with jax.named_scope("wait_far"):
        for copy in far:
            copy.wait()

    def swap_rows(out_rows, in_rows, which):
        def row_to(steps):
            return pltpu.make_async_remote_copy(
                src_ref=out_rows.at[lax.rem(me + steps, group)], dst_ref=in_rows.at[me],
                send_sem=row_send.at[which], recv_sem=row_recv.at[which],
                device_id=other(steps), device_id_type=MESH)

        own = pltpu.make_async_copy(out_rows.at[me], in_rows.at[me], row_own.at[which])
        own.start()
        half = group // 2
        row_to(half).start()

        def send(steps):
            row_to(half - steps).start()
            row_to(half + steps).start()

        each(1, half, send, 7)

        def finish():
            own.wait()
            every = pltpu.make_async_remote_copy(
                src_ref=out_rows.at[pl.ds(0, group - 1)], dst_ref=in_rows.at[pl.ds(0, group - 1)],
                send_sem=row_send.at[which], recv_sem=row_recv.at[which],
                device_id=other(half), device_id_type=MESH)
            every.wait()

        return finish

    def pairs(first, last):
        def body(tile, carry):
            pair_tile(tile, packet_ref, slab_start, coupling_ref[0], lists_ref, near_table,
                      source_table, home_table, real_ref)
            return carry

        lax.fori_loop(first, last, body, 0, unroll=4)

    table, tablet = table_ref[...], tablet_ref[...]
    value = spread_out[0] + far_in[...] + jnp.where(odd == 0, 0.0, near_in[0])
    rows = dot3(jnp.concatenate([value[0], value[1]], axis=1), table)
    columns = dot3(tablet, jnp.concatenate([rows[:, :full_z], rows[:, full_z:]], axis=0))
    there_out[:, 0, :] = columns[:full_y]
    there_out[:, 1, :] = columns[full_y:]
    with jax.named_scope("send_there"):
        finish = swap_rows(there_out, there_in, 0)

    for copy in visits:
        copy.wait()
    is_first = jnp.where(me == 0, 1.0, 0.0)
    is_last = jnp.where(me == group - 1, 1.0, 0.0)
    pair_ghosts(slab_start, float(full_x), ghost_in.at[0], ghost_in.at[1], is_first, is_last, tiles,
                near_table, source_table)
    with jax.named_scope("pairs_a"):
        pairs(0, windows[0])
    with jax.named_scope("prepare_c"):
        prepare(5, base_ref.shape[1] // ATOMS_AT_ONCE)
    with jax.named_scope("wait_there"):
        finish()

    columns = dot3(tablet, jnp.concatenate([there_in[:, 0, :], there_in[:, 1, :]], axis=0))
    gain = influence_ref[...] * scale
    columns = dot3(table, columns * jnp.concatenate([gain, gain], axis=0))
    back_out[:, 0, :] = columns[:full_x]
    back_out[:, 1, :] = columns[full_x:]
    with jax.named_scope("send_back"):
        finish = swap_rows(back_out, back_in, 1)
    with jax.named_scope("pairs_b"):
        pairs(windows[0], windows[1])
    with jax.named_scope("wait_back"):
        finish()

    columns = dot3(table, jnp.concatenate([back_in[:, 0, :], back_in[:, 1, :]], axis=0))
    rows = dot3(jnp.concatenate([columns[:full_y], columns[full_y:]], axis=1), tablet)
    plane_in[0, 0] = rows[:, :full_z]
    plane_in[0, 1] = rows[:, full_z:]
    lend_two = [carry_to(other(-2), plane_in.at[0, s], plane_in.at[2, s], plane_send, plane_recv, s)
                for s in range(2)]
    lend_three = [carry_to(other(-1), plane_in.at[2, s], plane_in.at[3, s], plane_send, plane_recv,
                           2 + s) for s in range(2)]
    lend_one, pass_one = (
        [carry_to(partner, plane_in.at[at, s], plane_in.at[1, s], plane_send, plane_recv, 4 + s)
         for s in range(2)] for at in (0, 2))
    for copy in lend_two:
        copy.start()

    @pl.when(odd == 1)
    def _():
        for copy in lend_one:
            copy.start()

    with jax.named_scope("pairs_c"):
        pairs(windows[1], windows[2])
    with jax.named_scope("wait_two"):
        for s in range(2):
            lend_two[s].wait()
            lend_three[s].start()

            @pl.when(odd == 0)
            def _():
                pass_one[s].start()

    with jax.named_scope("pairs_d"):
        pairs(windows[2], tiles)
    with jax.named_scope("wait_three"):
        for copy in lend_three + lend_one:
            copy.wait()
    with jax.named_scope("gather"):
        gather_atoms(ATOMS_AT_ONCE, spline_ref, slope_ref, plane_in, rows_y, slope_y, wide_z, low_z,
                     out_ref, planes)


def run_step(group, coupling, lists, charge_a, charge_b, positions, grid_base, spline, slope, ghosts,
             influence):
    order = spline.shape[1]
    full_x, full_z = influence.shape
    full_y = group
    atoms = positions.shape[1]
    tiles = lists.shape[1]
    visitors = ghosts.shape[1]
    every = tiles + 2 * (visitors // TILE)
    plane = (2, full_y, full_z)
    table, tablet = (jnp.asarray(value) for value in dft_tables(full_x))
    windows = (tiles * 3 // 8, tiles * 6 // 8, tiles * 7 // 8)
    inputs = (charge_a, charge_b, grid_base, spline, positions, ghosts, slope, table, tablet, influence)
    return pl.pallas_call(
        functools.partial(step_kernel, group, windows, 1.0 / (full_x * full_y * full_z)),
        out_shape=[f32(3, atoms)] * 2,
        in_specs=[SM] * 2 + [pl.BlockSpec(memory_space=pl.ANY)] * len(inputs),
        out_specs=[VM] * 2,
        scratch_shapes=[pltpu.VMEM(value.shape, value.dtype) for value in inputs] + [
            pltpu.SemaphoreType.DMA((len(inputs),)),
            pltpu.VMEM((full_y, atoms), jnp.float32),
            pltpu.VMEM((full_y, atoms), jnp.float32),
            pltpu.VMEM((2 * full_z, 2 * atoms), jnp.float32),
            pltpu.VMEM((2 * full_z, 2 * atoms), jnp.float32),
            pltpu.VMEM((8, atoms), jnp.float32),
            pltpu.VMEM((2 * full_y, order * full_z), jnp.float32),
            pltpu.VMEM((2 * order * full_y, 2 * full_z), jnp.float32),
            pltpu.VMEM((order, *plane), jnp.float32),
            pltpu.VMEM((2, *plane), jnp.float32),
            pltpu.VMEM(plane, jnp.float32),
            pltpu.VMEM(plane, jnp.float32),
            pltpu.VMEM((2, 8, visitors), jnp.float32),
            pltpu.VMEM((2, 8, visitors), jnp.float32),
            pltpu.VMEM((group, 2, full_z), jnp.float32),
            pltpu.VMEM((group, 2, full_z), jnp.float32),
            pltpu.VMEM((group, 2, full_z), jnp.float32),
            pltpu.VMEM((group, 2, full_z), jnp.float32),
            pltpu.VMEM((order, *plane), jnp.float32),
            pltpu.VMEM((every, TILE, TILE), jnp.float32),
            pltpu.VMEM((every, 32, TILE), jnp.float32),
            pltpu.VMEM((tiles, 32, TILE), jnp.float32),
            pltpu.SemaphoreType.DMA((4,)),
            pltpu.SemaphoreType.DMA((4,)),
            pltpu.SemaphoreType.DMA((2,)),
            pltpu.SemaphoreType.DMA((2,)),
            pltpu.SemaphoreType.DMA((2,)),
            pltpu.SemaphoreType.DMA((2,)),
            pltpu.SemaphoreType.DMA((2,)),
            pltpu.SemaphoreType.DMA((2,)),
            pltpu.SemaphoreType.DMA((2,)),
            pltpu.SemaphoreType.DMA((6,)),
            pltpu.SemaphoreType.DMA((6,)),
        ],
        compiler_params=pltpu.CompilerParams(
            vmem_limit_bytes=VMEM_LIMIT, collective_id=0, has_side_effects=True),
    )(coupling, lists, *inputs)


def per_device(charge_a, charge_b, coupling, positions, grid_base, spline, spline_slope, influence,
               pair_tiles, ghost_lists):
    group = lax.axis_size("px")
    reciprocal, real_space = run_step(
        group, coupling, pair_tiles.T, charge_a[None], charge_b[None], positions, grid_base, spline,
        spline_slope, ghost_lists, influence[:, 0])
    return reciprocal + real_space


def solution(mesh):
    placed = (
        P(("win", "px")),
        P(("win", "px")),
        P("win"),
        P(None, ("win", "px")),
        P(None, ("win", "px")),
        P(None, None, ("win", "px")),
        P(None, None, ("win", "px")),
        P(None, "px", None),
        P(("win", "px"), None),
        P(None, ("win", "px")),
    )
    return jax.shard_map(
        per_device, mesh=mesh, in_specs=placed, out_specs=P(None, ("win", "px")), check_vma=False
    )
```

```python
import functools
import math
import numpy as np
import jax
import jax.numpy as jnp
from jax import lax
from jax.experimental import pallas as pl
from jax.experimental.pallas import tpu as pltpu
from jax.sharding import PartitionSpec as P

TILE = 128
beta = 0.35
soften_sq = 0.25
VMEM_LIMIT = 60 * 1024 * 1024


def low_part(value):
    return value - value.astype(jnp.bfloat16).astype(jnp.float32)


def three_parts(value):
    first = value.astype(jnp.bfloat16).astype(jnp.float32)
    rest = value - first
    second = rest.astype(jnp.bfloat16).astype(jnp.float32)
    return first, second, rest - second


def dot(left, right, dims=((1,), (0,))):
    return lax.dot_general(left, right, (dims, ((), ())), preferred_element_type=jnp.float32)


def dot3(left, right):
    return dot(left, right) + (dot(low_part(left), right) + dot(left, low_part(right)))


def spline_columns(base_row, weights, length):
    lanes = base_row.shape[1]
    cells = lax.broadcasted_iota(jnp.int32, (length, lanes), 0)
    offset = (cells - base_row) & (length - 1)
    results = []
    for table in weights:
        value = jnp.zeros((length, lanes), jnp.float32)
        for step in reversed(range(len(table))):
            value = jnp.where(offset == step, table[step], value)
        results.append(value)
    return results


def dft_tables(length):
    index = np.arange(length)
    angle = 2.0 * np.pi * ((index[:, None] * index[None, :]) % length) / length
    cosine, sine = np.cos(angle), np.sin(angle)
    forward = np.block([[cosine, -sine], [sine, cosine]]).astype(np.float32)
    return forward, np.ascontiguousarray(forward.T)


def sum_tiles(value):
    rows, lanes = value.shape
    return jnp.sum(value.reshape(rows // 8, 8, lanes), axis=0)


def pair_features(scaled, home):
    first, second, third = three_parts(scaled)
    square = jnp.sum(scaled * scaled, axis=0, keepdims=True)
    ones = jnp.ones_like(square)
    if home:
        square = three_parts(square + soften_sq * beta * beta)
        rows = [first, first, second, second, first, third, *square, ones, ones, ones]
    else:
        square = three_parts(square)
        rows = [-2.0 * part for part in (first, second, first, second, third, first)]
        rows = rows + [ones, ones, ones, *square]
    rows.append(jnp.zeros((8, scaled.shape[1]), jnp.float32))
    return jnp.concatenate(rows, axis=0)


def pair_place(rows, shift, first_tile, near_table, source_table, home_table):
    local = jnp.concatenate([rows[0:1] + (shift - 0.5), rows[1:3] - 4.0], axis=0)
    scaled = local * beta
    q_a, q_b = rows[3:4], rows[4:5]
    source = jnp.concatenate([q_a, q_a * local, q_b, q_b * local], axis=0)
    source = jnp.concatenate([*three_parts(source), jnp.zeros_like(source)], axis=0)
    near = pair_features(scaled, False)
    near = jnp.concatenate([near, near, jnp.zeros((64, rows.shape[1]), jnp.float32)], axis=0)
    home = None if home_table is None else pair_features(scaled, True)
    for tile in range(rows.shape[1] // TILE):
        part = slice(tile * TILE, (tile + 1) * TILE)
        near_table[first_tile + tile] = near[:, part].T
        source_table[first_tile + tile] = source[:, part]
        if home is not None:
            home_table[first_tile + tile] = home[:, part]


def pair_own(slab_start, packet_ref, near_table, source_table, home_table, width=512):
    def own(step, carry):
        at = pl.ds(pl.multiple_of(step * width, width), width)
        pair_place(packet_ref[:, at], -slab_start, step * (width // TILE), near_table, source_table,
                   home_table)
        return carry

    lax.fori_loop(0, packet_ref.shape[1] // width, own, 0)


def pair_ghosts(slab_start, length, left_ref, right_ref, is_first, is_last, tiles, near_table,
                source_table):
    extra = left_ref.shape[1] // TILE
    pair_place(left_ref[...], -slab_start - is_first * length, tiles, near_table, source_table, None)
    pair_place(right_ref[...], -slab_start + is_last * length, tiles + extra, near_table,
               source_table, None)


def pair_tile(tile, packet_ref, slab_start, weight_b, lists_ref, near_table, source_table, home_table,
              out_ref):
    slots = lists_ref.shape[0]
    at = pl.ds(pl.multiple_of(tile * TILE, TILE), TILE)
    home = home_table[tile]
    blank = jnp.zeros_like(home)
    rest = jnp.zeros((TILE - 2 * home.shape[0], 2 * TILE), jnp.float32)
    wide_home = jnp.concatenate(
        [jnp.concatenate([home, blank], axis=1), jnp.concatenate([blank, home], axis=1), rest], axis=0)
    lane = lax.broadcasted_iota(jnp.int32, (TILE, TILE), 1)
    total = jnp.zeros((32, 2 * TILE), jnp.float32)
    for slot in range(0, slots, 2):
        one, two = lists_ref[slot, tile], lists_ref[slot + 1, tile]
        near = jnp.where(lane < 32, near_table[one], near_table[two])
        source = jnp.concatenate([source_table[one], source_table[two]], axis=1)
        square = dot(near, wide_home)
        inverse = lax.rsqrt(square)
        tail = (1.0 - lax.erf(square * inverse)) * inverse
        gauss = jnp.exp2(square * (-1.0 / math.log(2.0))) * (2.0 / math.sqrt(math.pi))
        radial = (tail + gauss) * (inverse * inverse)
        low = low_part(radial)
        both = jnp.concatenate(
            [jnp.concatenate([radial[:, :TILE], low[:, :TILE]], axis=1),
             jnp.concatenate([radial[:, TILE:], low[:, TILE:]], axis=1)], axis=0)
        total = total + dot(source, both)
    sums = total[:, :TILE] + total[:, TILE:]
    sums = sums[0:8] + sums[8:16] + sums[16:24]
    rows = packet_ref[:, at]
    local = jnp.concatenate([rows[0:1] - (slab_start + 0.5), rows[1:3] - 4.0], axis=0)
    scale = beta ** 3
    part_a = local * sums[0:1] - sums[1:4]
    part_b = local * sums[4:5] - sums[5:8]
    out_ref[:, at] = (
        ((1.0 - weight_b) * scale) * rows[3:4] * part_a + (weight_b * scale) * rows[4:5] * part_b)


VM = pl.BlockSpec(memory_space=pltpu.VMEM)
SM = pl.BlockSpec(memory_space=pltpu.SMEM)
params = pltpu.CompilerParams(vmem_limit_bytes=VMEM_LIMIT)


def f32(*shape):
    return jax.ShapeDtypeStruct(shape, jnp.float32)


def spread_atoms(chunk, charge_refs, base_ref, spline_ref, spread_out, grid_sum):
    order, _, full_y, full_z = spread_out.shape
    grid_sum[...] = jnp.zeros_like(grid_sum)

    def body(step, carry):
        at = pl.ds(pl.multiple_of(step * chunk, chunk), chunk)
        base = base_ref[:, at]
        weights = spline_ref[:, :, at]
        rows_y, = spline_columns(base[1:2], [[weights[1, o][None] for o in range(order)]], full_y)
        rows_z, = spline_columns(base[2:3], [[weights[2, o][None] for o in range(order)]], full_z)
        left = jnp.concatenate([ref[:, at] * rows_y for ref in charge_refs], axis=0)
        right = jnp.concatenate([weights[0, layer][None] * rows_z for layer in range(order)], axis=0)
        high = dot(jnp.concatenate([left, low_part(left)], axis=0), right, ((1,), (1,)))
        rest = dot(left, low_part(right), ((1,), (1,)))
        grid_sum[...] += high[:2 * full_y] + high[2 * full_y:] + rest
        return carry

    lax.fori_loop(0, base_ref.shape[1] // chunk, body, 0)
    for state in range(2):
        for layer in range(order):
            spread_out[layer, state] = grid_sum[state * full_y:(state + 1) * full_y,
                                                layer * full_z:(layer + 1) * full_z]


def gather_prepare(chunk, weight_b, charge_refs, base_ref, spline_ref, slope_ref, rows_y_ref,
                   slope_y_ref, wide_ref, low_ref, first, last):
    full_y = rows_y_ref.shape[0]
    order = spline_ref.shape[1]

    def body(step, carry):
        at = pl.ds(pl.multiple_of(step * chunk, chunk), chunk)
        twice = pl.ds(pl.multiple_of(step * 2 * chunk, 2 * chunk), 2 * chunk)
        base = base_ref[:, at]
        weights = spline_ref[:, :, at]
        slopes = slope_ref[:, :, at]

        def both(axis):
            return spline_columns(
                base[axis:axis + 1],
                [[table[axis, o][None] for o in range(order)] for table in (weights, slopes)],
                full_y)

        rows_y_ref[:, at], slope_y_ref[:, at] = both(1)
        stacked_z = jnp.concatenate(both(2), axis=1)
        scales = [(weight_b - 1.0) * charge_refs[0][:, at], -weight_b * charge_refs[1][:, at]]
        wide = jnp.concatenate(
            [jnp.concatenate([scale, scale], axis=1) * stacked_z for scale in scales], axis=0)
        wide_ref[:, twice] = wide
        low_ref[:, twice] = low_part(wide)
        return carry

    lax.fori_loop(first, last, body, 0)


def gather_layers(chunk, unroll, layers, before, spline_ref, slope_ref, plane_ref, rows_y_ref, slope_y_ref,
                  wide_ref, low_ref, out_ref, planes):
    _, _, full_y, full_z = plane_ref.shape
    height = len(layers) * full_y
    top = before * 2 * full_y
    for state in range(2):
        lanes = slice(state * full_z, (state + 1) * full_z)
        for place, layer in enumerate(layers):
            value = plane_ref[layer, state]
            first = top + place * full_y
            planes[first:first + full_y, lanes] = value
            planes[first + height:first + height + full_y, lanes] = low_part(value)

    def body(step, carry):
        at = pl.ds(pl.multiple_of(step * chunk, chunk), chunk)
        twice = pl.ds(pl.multiple_of(step * 2 * chunk, 2 * chunk), 2 * chunk)
        weights = spline_ref[0, :, at]
        slopes = slope_ref[0, :, at]
        rows_y, slope_y = rows_y_ref[:, at], slope_y_ref[:, at]
        high = dot(planes[top:top + 2 * height, :], wide_ref[:, twice])
        rest = dot(planes[top:top + height, :], low_ref[:, twice])
        sums = [jnp.zeros((8, chunk), jnp.float32) for _ in range(3)]
        for place, layer in enumerate(layers):
            part = slice(place * full_y, (place + 1) * full_y)
            again = slice(height + place * full_y, height + (place + 1) * full_y)
            sampled = high[part] + high[again] + rest[part]
            plain, sloped = sampled[:, :chunk], sampled[:, chunk:]
            plain_x, slope_x = weights[layer:layer + 1], slopes[layer:layer + 1]
            sums[0] = sums[0] + slope_x * sum_tiles(plain * rows_y)
            sums[1] = sums[1] + plain_x * sum_tiles(plain * slope_y)
            sums[2] = sums[2] + plain_x * sum_tiles(sloped * rows_y)
        for axis in range(3):
            result = jnp.sum(sums[axis], axis=0, keepdims=True)
            if before:
                result = result + out_ref[axis:axis + 1, at]
            out_ref[axis:axis + 1, at] = result
        return carry

    lax.fori_loop(0, spline_ref.shape[2] // chunk, body, 0)

MESH = pl.DeviceIdType.MESH
ATOMS_AT_ONCE = 512


def each(first, last, body, width):
    head = (last - first) % width
    for step in range(head):
        body(first + step)

    def block(index, carry):
        for step in range(width):
            body(first + head + index * width + step)
        return carry

    lax.fori_loop(0, (last - first - head) // width, block, 0)


def pick_ghosts(chunk, packet_ref, ghost_ref, ghost_out):
    height, atoms = packet_ref.shape
    ghosts = ghost_ref.shape[1]

    def pick(step, carry):
        at = pl.ds(pl.multiple_of(step * chunk, chunk), chunk)
        parts = jnp.concatenate(three_parts(packet_ref[:, at]), axis=0)
        ids = lax.broadcasted_iota(jnp.int32, (chunk, ghosts), 0) + step * chunk
        results = []
        for side in range(2):
            chosen = jnp.where(ids == ghost_ref[side:side + 1, :], 1.0, 0.0)
            results.append(carry[side] + dot(parts, chosen))
        return tuple(results)

    start = jnp.zeros((3 * height, ghosts), jnp.float32)
    sides = lax.fori_loop(0, atoms // chunk, pick, (start, start))
    for side, value in enumerate(sides):
        ghost_out[side] = value[:height] + value[height:2 * height] + value[2 * height:]


def step_kernel(group, scale, coupling_ref, lists_ref, *refs):
    inputs, (out_ref, real_ref), held, refs = refs[:14], refs[14:16], refs[16:30], refs[30:]
    (charge_a_ref, charge_b_ref, base_ref, spline_ref, position_ref, ghost_ref, slope_ref, influence_ref,
     table_ref, tablet_ref, table_rows_ref, tablet_rows_ref, table_columns_ref, tablet_columns_ref) = held
    (input_sem, rows_y, slope_y, wide_z, low_z, packet_ref, grid_sum, planes, spread_out, near_in, far_out, far_in, ghost_out, ghost_in, there_cross, there_out, there_in,
     back_cross, back_out, back_in,
     plane_in, near_table, source_table, home_table,
     near_send, near_recv, far_send, far_recv, ghost_send, ghost_recv, cross_send, cross_recv, row_send, row_recv,
     row_own,
     plane_send, plane_recv) = refs
    loads = [pltpu.make_async_copy(src, dst, input_sem.at[index])
             for index, (src, dst) in enumerate(zip(inputs, held))]
    for copy in loads:
        copy.start()
    me = lax.axis_index("px")
    order, _, full_y, full_z = spread_out.shape
    full_x = influence_ref.shape[0]
    tiles = lists_ref.shape[1]
    slab_start = me.astype(jnp.float32)

    def other(steps):
        return {"px": lax.rem(me + (steps + group), group)}

    barrier = pltpu.get_barrier_semaphore()

    def greet(steps):
        pl.semaphore_signal(barrier, inc=1, device_id=other(steps), device_id_type=MESH)

    chips = group // 2
    half = chips // 2

    with jax.named_scope("greet"):
        greet(2 * half)

        def greet_both(steps):
            greet(2 * (half - steps))
            greet(2 * (half + steps))

        each(1, half, greet_both, 5)
        greet(1)
        greet(-1)

    charge_refs = (charge_a_ref, charge_b_ref)
    for copy in loads[:4]:
        copy.wait()
    with jax.named_scope("spread"):
        spread_atoms(2048, charge_refs, base_ref, spline_ref, spread_out, grid_sum)

    with jax.named_scope("barrier_wait"):
        pl.semaphore_wait(barrier, chips + 1)

    odd = lax.rem(me, 2)
    partner = other(1 - 2 * odd)

    def carry_to(device, src, dst, sends, recvs, at):
        return pltpu.make_async_remote_copy(
            src_ref=src, dst_ref=dst, send_sem=sends.at[at], recv_sem=recvs.at[at],
            device_id=device, device_id_type=MESH)

    third = [carry_to(other(1), spread_out.at[3, s], near_in.at[1, s], near_send, near_recv, 2 + s)
             for s in range(2)]
    first = [carry_to(partner, spread_out.at[1, s], near_in.at[0, s], near_send, near_recv, s)
             for s in range(2)]
    far = [carry_to(other(2), far_out.at[s], far_in.at[s], far_send, far_recv, s) for s in range(2)]
    visits = [carry_to(other(1 - 2 * side), ghost_out.at[side], ghost_in.at[side], ghost_send,
                       ghost_recv, side) for side in range(2)]
    for copy in third + first:
        copy.start()
    for copy in loads[4:7]:
        copy.wait()
    with jax.named_scope("pick"):
        packet_ref[0:3, :] = position_ref[...]
        packet_ref[3:4, :] = charge_a_ref[...]
        packet_ref[4:5, :] = charge_b_ref[...]
        packet_ref[5:8, :] = jnp.zeros_like(position_ref)
        pick_ghosts(512, packet_ref, ghost_ref, ghost_out)
    prepare = functools.partial(gather_prepare, ATOMS_AT_ONCE, coupling_ref[0], charge_refs, base_ref,
                                spline_ref, slope_ref, rows_y, slope_y, wide_z, low_z)
    for copy in visits:
        copy.start()
    with jax.named_scope("wait_near"):
        for s in range(2):
            first[s].wait()
            third[s].wait()
            far_out[s] = spread_out[2, s] + near_in[1, s] + jnp.where(odd == 0, near_in[0, s], 0.0)
            far[s].start()
    with jax.named_scope("prepare_a"):
        prepare(0, 2)
    with jax.named_scope("pair_own"):
        pair_own(slab_start, packet_ref, near_table, source_table, home_table)
    with jax.named_scope("prepare_b"):
        prepare(2, 6)
    with jax.named_scope("wait_far"):
        for copy in far:
            copy.wait()

    chip = lax.div(me, 2)

    def swap_rows(columns, cross, paired, in_rows, which):
        upper, lower = columns[:group], columns[group:]
        mine = jnp.where(odd == 0, upper, lower)
        theirs = jnp.where(odd == 0, lower, upper)
        for part in range(2):
            rows_at = slice(part * chips, (part + 1) * chips)
            cross[:, part, :] = theirs[rows_at]
            paired[:, odd, part, :] = mine[rows_at]
        over = carry_to(partner, cross, paired.at[:, odd], cross_send, cross_recv, which)
        over.start()

        def row_to(steps):
            return pltpu.make_async_remote_copy(
                src_ref=paired.at[lax.rem(chip + steps, chips)], dst_ref=in_rows.at[chip],
                send_sem=row_send.at[which], recv_sem=row_recv.at[which],
                device_id=other(2 * steps), device_id_type=MESH)

        own = pltpu.make_async_copy(paired.at[chip], in_rows.at[chip], row_own.at[which])

        def send(steps):
            row_to(half - steps).start()
            row_to(half + steps).start()

        def go():
            over.wait()
            own.start()
            row_to(half).start()
            each(1, half, send, 5)

        def finish():
            own.wait()
            every = pltpu.make_async_remote_copy(
                src_ref=paired.at[pl.ds(0, chips - 1)], dst_ref=in_rows.at[pl.ds(0, chips - 1)],
                send_sem=row_send.at[which], recv_sem=row_recv.at[which],
                device_id=other(2 * half), device_id_type=MESH)
            every.wait()
            return jnp.concatenate(
                [in_rows[:, side, part, :] for side in range(2) for part in range(2)], axis=0)

        return go, finish

    def pairs(first, last):
        def body(tile, carry):
            pair_tile(tile, packet_ref, slab_start, coupling_ref[0], lists_ref, near_table,
                      source_table, home_table, real_ref)
            return carry

        lax.fori_loop(first, last, body, 0, unroll=4)

    for copy in loads[7:]:
        copy.wait()
    value = spread_out[0] + far_in[...] + jnp.where(odd == 0, 0.0, near_in[0])
    rows = dot3(jnp.concatenate([value[0], value[1]], axis=1), table_ref[...])
    rows = jnp.concatenate([rows[:, :full_z], rows[:, full_z:]], axis=0)
    go, finish = swap_rows(dot3(tablet_rows_ref[...], rows), there_cross, there_out, there_in, 0)
    with jax.named_scope("send_there"):
        go()
    with jax.named_scope("ghosts"):
        for copy in visits:
            copy.wait()
        is_first = jnp.where(me == 0, 1.0, 0.0)
        is_last = jnp.where(me == group - 1, 1.0, 0.0)
        pair_ghosts(slab_start, float(full_x), ghost_in.at[0], ghost_in.at[1], is_first, is_last,
                    tiles, near_table, source_table)
    with jax.named_scope("pairs_a"):
        pairs(0, tiles * 3 // 8)
    with jax.named_scope("prepare_c"):
        prepare(6, base_ref.shape[1] // ATOMS_AT_ONCE)
    with jax.named_scope("wait_there"):
        columns = finish()

    columns = dot3(tablet_columns_ref[...], columns)
    gain = influence_ref[...] * scale
    columns = dot3(table_rows_ref[...], columns * jnp.concatenate([gain, gain], axis=0))
    go, finish = swap_rows(columns, back_cross, back_out, back_in, 1)
    with jax.named_scope("send_back"):
        go()
    with jax.named_scope("pairs_b"):
        pairs(tiles * 3 // 8, tiles)
    with jax.named_scope("wait_back"):
        columns = finish()

    columns = dot3(table_columns_ref[...], columns)
    rows = dot3(jnp.concatenate([columns[:full_y], columns[full_y:]], axis=1), tablet_ref[...])
    plane_in[0, 0] = rows[:, :full_z]
    plane_in[0, 1] = rows[:, full_z:]
    lend_two = [carry_to(other(-2), plane_in.at[0, s], plane_in.at[2, s], plane_send, plane_recv, s)
                for s in range(2)]
    lend_three = [carry_to(other(-1), plane_in.at[2, s], plane_in.at[3, s], plane_send, plane_recv,
                           2 + s) for s in range(2)]
    lend_one, pass_one = (
        [carry_to(partner, plane_in.at[at, s], plane_in.at[1, s], plane_send, plane_recv, 4 + s)
         for s in range(2)] for at in (0, 2))
    for copy in lend_two:
        copy.start()

    @pl.when(odd == 1)
    def _():
        for copy in lend_one:
            copy.start()

    def gather(layers, before):
        gather_layers(ATOMS_AT_ONCE, 4 // len(layers), layers, before, spline_ref, slope_ref, plane_in,
                      rows_y, slope_y, wide_z, low_z, out_ref, planes)

    with jax.named_scope("gather_a"):
        gather((0,), 0)
    with jax.named_scope("wait_two"):
        for s in range(2):
            lend_two[s].wait()
            lend_three[s].start()

            @pl.when(odd == 0)
            def _():
                pass_one[s].start()

    with jax.named_scope("gather_b"):
        gather((2,), 1)
    with jax.named_scope("wait_three"):
        for copy in lend_three + lend_one:
            copy.wait()
    with jax.named_scope("gather_c"):
        gather((1, 3), 2)


def run_step(group, coupling, lists, charge_a, charge_b, positions, grid_base, spline, slope, ghosts,
             influence):
    order = spline.shape[1]
    full_x, full_z = influence.shape
    full_y = group
    atoms = positions.shape[1]
    tiles = lists.shape[1]
    visitors = ghosts.shape[1]
    every = tiles + 2 * (visitors // TILE)
    plane = (2, full_y, full_z)
    tables = dft_tables(full_x)
    order_of = np.arange(full_x)
    sides = [order_of[side::2] + part * full_x for side in range(2) for part in range(2)]
    split = np.concatenate(sides)
    tables = tables + tuple(value[split] for value in tables) + tuple(value[:, split] for value in tables)
    inputs = (charge_a, charge_b, grid_base, spline, positions, ghosts, slope, influence,
              *(jnp.asarray(value) for value in tables))
    return pl.pallas_call(
        functools.partial(step_kernel, group, 1.0 / (full_x * full_y * full_z)),
        out_shape=[f32(3, atoms)] * 2,
        in_specs=[SM] * 2 + [pl.BlockSpec(memory_space=pl.ANY)] * len(inputs),
        out_specs=[VM] * 2,
        scratch_shapes=[pltpu.VMEM(value.shape, value.dtype) for value in inputs] + [
            pltpu.SemaphoreType.DMA((len(inputs),)),
            pltpu.VMEM((full_y, atoms), jnp.float32),
            pltpu.VMEM((full_y, atoms), jnp.float32),
            pltpu.VMEM((2 * full_z, 2 * atoms), jnp.float32),
            pltpu.VMEM((2 * full_z, 2 * atoms), jnp.float32),
            pltpu.VMEM((8, atoms), jnp.float32),
            pltpu.VMEM((2 * full_y, order * full_z), jnp.float32),
            pltpu.VMEM((2 * order * full_y, 2 * full_z), jnp.float32),
            pltpu.VMEM((order, *plane), jnp.float32),
            pltpu.VMEM((2, *plane), jnp.float32),
            pltpu.VMEM(plane, jnp.float32),
            pltpu.VMEM(plane, jnp.float32),
            pltpu.VMEM((2, 8, visitors), jnp.float32),
            pltpu.VMEM((2, 8, visitors), jnp.float32),
            *[pltpu.VMEM((group // 2, *sides, 2, full_z), jnp.float32)
              for sides in ((), (2,), (2,)) * 2],
            pltpu.VMEM((order, *plane), jnp.float32),
            pltpu.VMEM((every, TILE, TILE), jnp.float32),
            pltpu.VMEM((every, 32, TILE), jnp.float32),
            pltpu.VMEM((tiles, 32, TILE), jnp.float32),
            *[pltpu.SemaphoreType.DMA((count,)) for count in (4, 4, 2, 2, 2, 2, 2, 2, 2, 2, 2, 6, 6)],
        ],
        compiler_params=pltpu.CompilerParams(
            vmem_limit_bytes=VMEM_LIMIT, collective_id=0, has_side_effects=True),
    )(coupling, lists, *inputs)


def per_device(charge_a, charge_b, coupling, positions, grid_base, spline, spline_slope, influence,
               pair_tiles, ghost_lists):
    group = lax.axis_size("px")
    reciprocal, real_space = run_step(
        group, coupling, pair_tiles.T, charge_a[None], charge_b[None], positions, grid_base, spline,
        spline_slope, ghost_lists, influence[:, 0])
    return reciprocal + real_space


def solution(mesh):
    placed = (
        P(("win", "px")),
        P(("win", "px")),
        P("win"),
        P(None, ("win", "px")),
        P(None, ("win", "px")),
        P(None, None, ("win", "px")),
        P(None, None, ("win", "px")),
        P(None, "px", None),
        P(("win", "px"), None),
        P(None, ("win", "px")),
    )
    return jax.shard_map(
        per_device, mesh=mesh, in_specs=placed, out_specs=P(None, ("win", "px")), check_vma=False
    )
```

```python
import functools
import math
import numpy as np
import jax
import jax.numpy as jnp
from jax import lax
from jax.experimental import pallas as pl
from jax.experimental.pallas import tpu as pltpu
from jax.sharding import PartitionSpec as P

TILE = 128
beta = 0.35
soften_sq = 0.25
VMEM_LIMIT = 60 * 1024 * 1024


def low_part(value):
    return value - value.astype(jnp.bfloat16).astype(jnp.float32)


def three_parts(value):
    first = value.astype(jnp.bfloat16).astype(jnp.float32)
    rest = value - first
    second = rest.astype(jnp.bfloat16).astype(jnp.float32)
    return first, second, rest - second


def dot(left, right, dims=((1,), (0,))):
    return lax.dot_general(left, right, (dims, ((), ())), preferred_element_type=jnp.float32)


def dot3(left, right):
    return dot(left, right) + (dot(low_part(left), right) + dot(left, low_part(right)))


def spline_columns(base_row, weights, length):
    lanes = base_row.shape[1]
    cells = lax.broadcasted_iota(jnp.int32, (length, lanes), 0)
    offset = (cells - base_row) & (length - 1)
    results = []
    for table in weights:
        value = jnp.zeros((length, lanes), jnp.float32)
        for step in reversed(range(len(table))):
            value = jnp.where(offset == step, table[step], value)
        results.append(value)
    return results


def dft_tables(length):
    index = np.arange(length)
    angle = 2.0 * np.pi * ((index[:, None] * index[None, :]) % length) / length
    cosine, sine = np.cos(angle), np.sin(angle)
    forward = np.block([[cosine, -sine], [sine, cosine]]).astype(np.float32)
    return forward, np.ascontiguousarray(forward.T)


def sum_tiles(value):
    rows, lanes = value.shape
    return jnp.sum(value.reshape(rows // 8, 8, lanes), axis=0)


def pair_features(scaled, home):
    first, second, third = three_parts(scaled)
    square = jnp.sum(scaled * scaled, axis=0, keepdims=True)
    ones = jnp.ones_like(square)
    if home:
        square = three_parts(square + soften_sq * beta * beta)
        rows = [first, first, second, second, first, third, *square, ones, ones, ones]
    else:
        square = three_parts(square)
        rows = [-2.0 * part for part in (first, second, first, second, third, first)]
        rows = rows + [ones, ones, ones, *square]
    rows.append(jnp.zeros((8, scaled.shape[1]), jnp.float32))
    return jnp.concatenate(rows, axis=0)


def pair_place(rows, shift, first_tile, near_table, source_table, home_table):
    local = jnp.concatenate([rows[0:1] + (shift - 0.5), rows[1:3] - 4.0], axis=0)
    scaled = local * beta
    q_a, q_b = rows[3:4], rows[4:5]
    source = jnp.concatenate([q_a, q_a * local, q_b, q_b * local], axis=0)
    source = jnp.concatenate([*three_parts(source), jnp.zeros_like(source)], axis=0)
    near = pair_features(scaled, False)
    near = jnp.concatenate([near, near, jnp.zeros((64, rows.shape[1]), jnp.float32)], axis=0)
    home = None if home_table is None else pair_features(scaled, True)
    for tile in range(rows.shape[1] // TILE):
        part = slice(tile * TILE, (tile + 1) * TILE)
        near_table[first_tile + tile] = near[:, part].T
        source_table[first_tile + tile] = source[:, part]
        if home is not None:
            home_table[first_tile + tile] = home[:, part]


def pair_own(slab_start, packet_ref, near_table, source_table, home_table, width=512):
    def own(step, carry):
        at = pl.ds(pl.multiple_of(step * width, width), width)
        pair_place(packet_ref[:, at], -slab_start, step * (width // TILE), near_table, source_table,
                   home_table)
        return carry

    lax.fori_loop(0, packet_ref.shape[1] // width, own, 0)


def pair_ghosts(slab_start, length, left_ref, right_ref, is_first, is_last, tiles, near_table,
                source_table):
    extra = left_ref.shape[1] // TILE
    pair_place(left_ref[...], -slab_start - is_first * length, tiles, near_table, source_table, None)
    pair_place(right_ref[...], -slab_start + is_last * length, tiles + extra, near_table,
               source_table, None)


def pair_tile(tile, packet_ref, slab_start, weight_b, lists_ref, near_table, source_table, home_table,
              out_ref):
    slots = lists_ref.shape[0]
    at = pl.ds(pl.multiple_of(tile * TILE, TILE), TILE)
    home = home_table[tile]
    blank = jnp.zeros_like(home)
    rest = jnp.zeros((TILE - 2 * home.shape[0], 2 * TILE), jnp.float32)
    wide_home = jnp.concatenate(
        [jnp.concatenate([home, blank], axis=1), jnp.concatenate([blank, home], axis=1), rest], axis=0)
    lane = lax.broadcasted_iota(jnp.int32, (TILE, TILE), 1)
    total = jnp.zeros((32, 2 * TILE), jnp.float32)
    for slot in range(0, slots, 2):
        one, two = lists_ref[slot, tile], lists_ref[slot + 1, tile]
        near = jnp.where(lane < 32, near_table[one], near_table[two])
        source = jnp.concatenate([source_table[one], source_table[two]], axis=1)
        square = dot(near, wide_home)
        inverse = lax.rsqrt(square)
        tail = (1.0 - lax.erf(square * inverse)) * inverse
        gauss = jnp.exp2(square * (-1.0 / math.log(2.0))) * (2.0 / math.sqrt(math.pi))
        radial = (tail + gauss) * (inverse * inverse)
        low = low_part(radial)
        both = jnp.concatenate(
            [jnp.concatenate([radial[:, :TILE], low[:, :TILE]], axis=1),
             jnp.concatenate([radial[:, TILE:], low[:, TILE:]], axis=1)], axis=0)
        total = total + dot(source, both)
    sums = total[:, :TILE] + total[:, TILE:]
    sums = sums[0:8] + sums[8:16] + sums[16:24]
    rows = packet_ref[:, at]
    local = jnp.concatenate([rows[0:1] - (slab_start + 0.5), rows[1:3] - 4.0], axis=0)
    scale = beta ** 3
    part_a = local * sums[0:1] - sums[1:4]
    part_b = local * sums[4:5] - sums[5:8]
    out_ref[:, at] = (
        ((1.0 - weight_b) * scale) * rows[3:4] * part_a + (weight_b * scale) * rows[4:5] * part_b)


VM = pl.BlockSpec(memory_space=pltpu.VMEM)
SM = pl.BlockSpec(memory_space=pltpu.SMEM)
params = pltpu.CompilerParams(vmem_limit_bytes=VMEM_LIMIT)


def f32(*shape):
    return jax.ShapeDtypeStruct(shape, jnp.float32)


def spread_atoms(chunk, charge_refs, base_ref, spline_ref, spread_out, grid_sum):
    order, _, full_y, full_z = spread_out.shape
    grid_sum[...] = jnp.zeros_like(grid_sum)

    def body(step, carry):
        at = pl.ds(pl.multiple_of(step * chunk, chunk), chunk)
        base = base_ref[:, at]
        weights = spline_ref[:, :, at]
        rows_y, = spline_columns(base[1:2], [[weights[1, o][None] for o in range(order)]], full_y)
        rows_z, = spline_columns(base[2:3], [[weights[2, o][None] for o in range(order)]], full_z)
        left = jnp.concatenate([ref[:, at] * rows_y for ref in charge_refs], axis=0)
        right = jnp.concatenate([weights[0, layer][None] * rows_z for layer in range(order)], axis=0)
        high = dot(jnp.concatenate([left, low_part(left)], axis=0), right, ((1,), (1,)))
        rest = dot(left, low_part(right), ((1,), (1,)))
        grid_sum[...] += high[:2 * full_y] + high[2 * full_y:] + rest
        return carry

    lax.fori_loop(0, base_ref.shape[1] // chunk, body, 0)
    for state in range(2):
        for layer in range(order):
            spread_out[layer, state] = grid_sum[state * full_y:(state + 1) * full_y,
                                                layer * full_z:(layer + 1) * full_z]


def gather_prepare(chunk, weight_b, charge_refs, base_ref, spline_ref, slope_ref, rows_y_ref,
                   slope_y_ref, wide_ref, low_ref, first, last):
    full_y = rows_y_ref.shape[0]
    order = spline_ref.shape[1]

    def body(step, carry):
        at = pl.ds(pl.multiple_of(step * chunk, chunk), chunk)
        twice = pl.ds(pl.multiple_of(step * 2 * chunk, 2 * chunk), 2 * chunk)
        base = base_ref[:, at]
        weights = spline_ref[:, :, at]
        slopes = slope_ref[:, :, at]

        def both(axis):
            return spline_columns(
                base[axis:axis + 1],
                [[table[axis, o][None] for o in range(order)] for table in (weights, slopes)],
                full_y)

        rows_y_ref[:, at], slope_y_ref[:, at] = both(1)
        stacked_z = jnp.concatenate(both(2), axis=1)
        scales = [(weight_b - 1.0) * charge_refs[0][:, at], -weight_b * charge_refs[1][:, at]]
        wide = jnp.concatenate(
            [jnp.concatenate([scale, scale], axis=1) * stacked_z for scale in scales], axis=0)
        wide_ref[:, twice] = wide
        low_ref[:, twice] = low_part(wide)
        return carry

    lax.fori_loop(first, last, body, 0)


def gather_layers(chunk, unroll, layers, before, spline_ref, slope_ref, plane_ref, rows_y_ref, slope_y_ref,
                  wide_ref, low_ref, out_ref, planes):
    _, _, full_y, full_z = plane_ref.shape
    height = len(layers) * full_y
    top = before * 2 * full_y
    for state in range(2):
        lanes = slice(state * full_z, (state + 1) * full_z)
        for place, layer in enumerate(layers):
            value = plane_ref[layer, state]
            first = top + place * full_y
            planes[first:first + full_y, lanes] = value
            planes[first + height:first + height + full_y, lanes] = low_part(value)

    def body(step, carry):
        at = pl.ds(pl.multiple_of(step * chunk, chunk), chunk)
        twice = pl.ds(pl.multiple_of(step * 2 * chunk, 2 * chunk), 2 * chunk)
        weights = spline_ref[0, :, at]
        slopes = slope_ref[0, :, at]
        rows_y, slope_y = rows_y_ref[:, at], slope_y_ref[:, at]
        high = dot(planes[top:top + 2 * height, :], wide_ref[:, twice])
        rest = dot(planes[top:top + height, :], low_ref[:, twice])
        sums = [jnp.zeros((8, chunk), jnp.float32) for _ in range(3)]
        for place, layer in enumerate(layers):
            part = slice(place * full_y, (place + 1) * full_y)
            again = slice(height + place * full_y, height + (place + 1) * full_y)
            sampled = high[part] + high[again] + rest[part]
            plain, sloped = sampled[:, :chunk], sampled[:, chunk:]
            plain_x, slope_x = weights[layer:layer + 1], slopes[layer:layer + 1]
            sums[0] = sums[0] + slope_x * sum_tiles(plain * rows_y)
            sums[1] = sums[1] + plain_x * sum_tiles(plain * slope_y)
            sums[2] = sums[2] + plain_x * sum_tiles(sloped * rows_y)
        for axis in range(3):
            result = jnp.sum(sums[axis], axis=0, keepdims=True)
            if before:
                result = result + out_ref[axis:axis + 1, at]
            out_ref[axis:axis + 1, at] = result
        return carry

    lax.fori_loop(0, spline_ref.shape[2] // chunk, body, 0, unroll=unroll)

MESH = pl.DeviceIdType.MESH
ATOMS_AT_ONCE = 512


def each(first, last, body, width):
    head = (last - first) % width
    for step in range(head):
        body(first + step)

    def block(index, carry):
        for step in range(width):
            body(first + head + index * width + step)
        return carry

    lax.fori_loop(0, (last - first - head) // width, block, 0)


def pick_ghosts(chunk, packet_ref, ghost_ref, ghost_out):
    height, atoms = packet_ref.shape
    ghosts = ghost_ref.shape[1]

    def pick(step, carry):
        at = pl.ds(pl.multiple_of(step * chunk, chunk), chunk)
        parts = jnp.concatenate(three_parts(packet_ref[:, at]), axis=0)
        ids = lax.broadcasted_iota(jnp.int32, (chunk, ghosts), 0) + step * chunk
        results = []
        for side in range(2):
            chosen = jnp.where(ids == ghost_ref[side:side + 1, :], 1.0, 0.0)
            results.append(carry[side] + dot(parts, chosen))
        return tuple(results)

    start = jnp.zeros((3 * height, ghosts), jnp.float32)
    sides = lax.fori_loop(0, atoms // chunk, pick, (start, start))
    for side, value in enumerate(sides):
        ghost_out[side] = value[:height] + value[height:2 * height] + value[2 * height:]


def step_kernel(group, scale, coupling_ref, lists_ref, *refs):
    inputs, (out_ref, real_ref), held, refs = refs[:14], refs[14:16], refs[16:30], refs[30:]
    (charge_a_ref, charge_b_ref, base_ref, spline_ref, position_ref, ghost_ref, slope_ref, influence_ref,
     table_ref, tablet_ref, table_rows_ref, tablet_rows_ref, table_columns_ref, tablet_columns_ref) = held
    (input_sem, rows_y, slope_y, wide_z, low_z, packet_ref, grid_sum, planes, spread_out, near_in, far_out, far_in, ghost_out, ghost_in, there_cross, there_out, there_in,
     back_cross, back_out, back_in,
     plane_in, near_table, source_table, home_table,
     near_send, near_recv, far_send, far_recv, ghost_send, ghost_recv, cross_send, cross_recv, row_send, row_recv,
     row_own,
     plane_send, plane_recv) = refs
    loads = [pltpu.make_async_copy(src, dst, input_sem.at[index])
             for index, (src, dst) in enumerate(zip(inputs, held))]
    for copy in loads:
        copy.start()
    me = lax.axis_index("px")
    order, _, full_y, full_z = spread_out.shape
    full_x = influence_ref.shape[0]
    tiles = lists_ref.shape[1]
    slab_start = me.astype(jnp.float32)

    def other(steps):
        return {"px": lax.rem(me + (steps + group), group)}

    barrier = pltpu.get_barrier_semaphore()

    def greet(steps):
        pl.semaphore_signal(barrier, inc=1, device_id=other(steps), device_id_type=MESH)

    chips = group // 2
    half = chips // 2

    with jax.named_scope("greet"):
        greet(2 * half)

        def greet_both(steps):
            greet(2 * (half - steps))
            greet(2 * (half + steps))

        each(1, half, greet_both, 5)
        greet(1)
        greet(-1)

    charge_refs = (charge_a_ref, charge_b_ref)
    for copy in loads[:4]:
        copy.wait()
    with jax.named_scope("spread"):
        spread_atoms(2048, charge_refs, base_ref, spline_ref, spread_out, grid_sum)

    with jax.named_scope("barrier_wait"):
        pl.semaphore_wait(barrier, chips + 1)

    odd = lax.rem(me, 2)
    partner = other(1 - 2 * odd)

    def carry_to(device, src, dst, sends, recvs, at):
        return pltpu.make_async_remote_copy(
            src_ref=src, dst_ref=dst, send_sem=sends.at[at], recv_sem=recvs.at[at],
            device_id=device, device_id_type=MESH)

    third = [carry_to(other(1), spread_out.at[3, s], near_in.at[1, s], near_send, near_recv, 2 + s)
             for s in range(2)]
    first = [carry_to(partner, spread_out.at[1, s], near_in.at[0, s], near_send, near_recv, s)
             for s in range(2)]
    far = [carry_to(other(2), far_out.at[s], far_in.at[s], far_send, far_recv, s) for s in range(2)]
    visits = [carry_to(other(1 - 2 * side), ghost_out.at[side], ghost_in.at[side], ghost_send,
                       ghost_recv, side) for side in range(2)]
    for copy in third + first:
        copy.start()
    for copy in loads[4:7]:
        copy.wait()
    with jax.named_scope("pick"):
        packet_ref[0:3, :] = position_ref[...]
        packet_ref[3:4, :] = charge_a_ref[...]
        packet_ref[4:5, :] = charge_b_ref[...]
        packet_ref[5:8, :] = jnp.zeros_like(position_ref)
        pick_ghosts(512, packet_ref, ghost_ref, ghost_out)
    prepare = functools.partial(gather_prepare, ATOMS_AT_ONCE, coupling_ref[0], charge_refs, base_ref,
                                spline_ref, slope_ref, rows_y, slope_y, wide_z, low_z)
    for copy in visits:
        copy.start()
    with jax.named_scope("wait_near"):
        for s in range(2):
            first[s].wait()
            third[s].wait()
            far_out[s] = spread_out[2, s] + near_in[1, s] + jnp.where(odd == 0, near_in[0, s], 0.0)
            far[s].start()
    with jax.named_scope("prepare_a"):
        prepare(0, 2)
    with jax.named_scope("pair_own"):
        pair_own(slab_start, packet_ref, near_table, source_table, home_table)
    with jax.named_scope("prepare_b"):
        prepare(2, 6)
    with jax.named_scope("wait_far"):
        for copy in far:
            copy.wait()

    chip = lax.div(me, 2)

    def swap_rows(columns, cross, paired, in_rows, which):
        upper, lower = columns[:group], columns[group:]
        mine = jnp.where(odd == 0, upper, lower)
        theirs = jnp.where(odd == 0, lower, upper)
        for part in range(2):
            rows_at = slice(part * chips, (part + 1) * chips)
            cross[:, part, :] = theirs[rows_at]
            paired[:, odd, part, :] = mine[rows_at]
        over = carry_to(partner, cross, paired.at[:, odd], cross_send, cross_recv, which)
        over.start()

        def row_to(steps):
            return pltpu.make_async_remote_copy(
                src_ref=paired.at[lax.rem(chip + steps, chips)], dst_ref=in_rows.at[chip],
                send_sem=row_send.at[which], recv_sem=row_recv.at[which],
                device_id=other(2 * steps), device_id_type=MESH)

        own = pltpu.make_async_copy(paired.at[chip], in_rows.at[chip], row_own.at[which])

        def send(steps):
            row_to(half - steps).start()
            row_to(half + steps).start()

        def go():
            over.wait()
            own.start()
            row_to(half).start()
            each(1, half, send, 5)

        def finish():
            own.wait()
            every = pltpu.make_async_remote_copy(
                src_ref=paired.at[pl.ds(0, chips - 1)], dst_ref=in_rows.at[pl.ds(0, chips - 1)],
                send_sem=row_send.at[which], recv_sem=row_recv.at[which],
                device_id=other(2 * half), device_id_type=MESH)
            every.wait()
            return jnp.concatenate(
                [in_rows[:, side, part, :] for side in range(2) for part in range(2)], axis=0)

        return go, finish

    def pairs(first, last):
        def body(tile, carry):
            pair_tile(tile, packet_ref, slab_start, coupling_ref[0], lists_ref, near_table,
                      source_table, home_table, real_ref)
            return carry

        lax.fori_loop(first, last, body, 0, unroll=4)

    for copy in loads[7:]:
        copy.wait()
    value = spread_out[0] + far_in[...] + jnp.where(odd == 0, 0.0, near_in[0])
    rows = dot3(jnp.concatenate([value[0], value[1]], axis=1), table_ref[...])
    rows = jnp.concatenate([rows[:, :full_z], rows[:, full_z:]], axis=0)
    go, finish = swap_rows(dot3(tablet_rows_ref[...], rows), there_cross, there_out, there_in, 0)
    with jax.named_scope("send_there"):
        go()
    with jax.named_scope("ghosts"):
        for copy in visits:
            copy.wait()
        is_first = jnp.where(me == 0, 1.0, 0.0)
        is_last = jnp.where(me == group - 1, 1.0, 0.0)
        pair_ghosts(slab_start, float(full_x), ghost_in.at[0], ghost_in.at[1], is_first, is_last,
                    tiles, near_table, source_table)
    with jax.named_scope("pairs_a"):
        pairs(0, tiles // 2)
    with jax.named_scope("prepare_c"):
        prepare(6, base_ref.shape[1] // ATOMS_AT_ONCE)
    with jax.named_scope("wait_there"):
        columns = finish()

    columns = dot3(tablet_columns_ref[...], columns)
    gain = influence_ref[...] * scale
    columns = dot3(table_rows_ref[...], columns * jnp.concatenate([gain, gain], axis=0))
    go, finish = swap_rows(columns, back_cross, back_out, back_in, 1)
    with jax.named_scope("send_back"):
        go()
    with jax.named_scope("pairs_b"):
        pairs(tiles // 2, tiles)
    with jax.named_scope("wait_back"):
        columns = finish()

    columns = dot3(table_columns_ref[...], columns)
    rows = dot3(jnp.concatenate([columns[:full_y], columns[full_y:]], axis=1), tablet_ref[...])
    plane_in[0, 0] = rows[:, :full_z]
    plane_in[0, 1] = rows[:, full_z:]
    lend_two = [carry_to(other(-2), plane_in.at[0, s], plane_in.at[2, s], plane_send, plane_recv, s)
                for s in range(2)]
    lend_three = [carry_to(other(-1), plane_in.at[2, s], plane_in.at[3, s], plane_send, plane_recv,
                           2 + s) for s in range(2)]
    lend_one, pass_one = (
        [carry_to(partner, plane_in.at[at, s], plane_in.at[1, s], plane_send, plane_recv, 4 + s)
         for s in range(2)] for at in (0, 2))
    for copy in lend_two:
        copy.start()

    @pl.when(odd == 1)
    def _():
        for copy in lend_one:
            copy.start()

    def gather(layers, before):
        gather_layers(ATOMS_AT_ONCE, 4 // len(layers), layers, before, spline_ref, slope_ref, plane_in,
                      rows_y, slope_y, wide_z, low_z, out_ref, planes)

    with jax.named_scope("gather_a"):
        gather((0,), 0)
    with jax.named_scope("wait_two"):
        for s in range(2):
            lend_two[s].wait()
            lend_three[s].start()

            @pl.when(odd == 0)
            def _():
                pass_one[s].start()

    with jax.named_scope("gather_b"):
        gather((2,), 1)
    with jax.named_scope("wait_three"):
        for copy in lend_three + lend_one:
            copy.wait()
    with jax.named_scope("gather_c"):
        gather((1, 3), 2)


def run_step(group, coupling, lists, charge_a, charge_b, positions, grid_base, spline, slope, ghosts,
             influence):
    order = spline.shape[1]
    full_x, full_z = influence.shape
    full_y = group
    atoms = positions.shape[1]
    tiles = lists.shape[1]
    visitors = ghosts.shape[1]
    every = tiles + 2 * (visitors // TILE)
    plane = (2, full_y, full_z)
    tables = dft_tables(full_x)
    order_of = np.arange(full_x)
    sides = [order_of[side::2] + part * full_x for side in range(2) for part in range(2)]
    split = np.concatenate(sides)
    tables = tables + tuple(value[split] for value in tables) + tuple(value[:, split] for value in tables)
    inputs = (charge_a, charge_b, grid_base, spline, positions, ghosts, slope, influence,
              *(jnp.asarray(value) for value in tables))
    return pl.pallas_call(
        functools.partial(step_kernel, group, 1.0 / (full_x * full_y * full_z)),
        out_shape=[f32(3, atoms)] * 2,
        in_specs=[SM] * 2 + [pl.BlockSpec(memory_space=pl.ANY)] * len(inputs),
        out_specs=[VM] * 2,
        scratch_shapes=[pltpu.VMEM(value.shape, value.dtype) for value in inputs] + [
            pltpu.SemaphoreType.DMA((len(inputs),)),
            pltpu.VMEM((full_y, atoms), jnp.float32),
            pltpu.VMEM((full_y, atoms), jnp.float32),
            pltpu.VMEM((2 * full_z, 2 * atoms), jnp.float32),
            pltpu.VMEM((2 * full_z, 2 * atoms), jnp.float32),
            pltpu.VMEM((8, atoms), jnp.float32),
            pltpu.VMEM((2 * full_y, order * full_z), jnp.float32),
            pltpu.VMEM((2 * order * full_y, 2 * full_z), jnp.float32),
            pltpu.VMEM((order, *plane), jnp.float32),
            pltpu.VMEM((2, *plane), jnp.float32),
            pltpu.VMEM(plane, jnp.float32),
            pltpu.VMEM(plane, jnp.float32),
            pltpu.VMEM((2, 8, visitors), jnp.float32),
            pltpu.VMEM((2, 8, visitors), jnp.float32),
            *[pltpu.VMEM((group // 2, *sides, 2, full_z), jnp.float32)
              for sides in ((), (2,), (2,)) * 2],
            pltpu.VMEM((order, *plane), jnp.float32),
            pltpu.VMEM((every, TILE, TILE), jnp.float32),
            pltpu.VMEM((every, 32, TILE), jnp.float32),
            pltpu.VMEM((tiles, 32, TILE), jnp.float32),
            *[pltpu.SemaphoreType.DMA((count,)) for count in (4, 4, 2, 2, 2, 2, 2, 2, 2, 2, 2, 6, 6)],
        ],
        compiler_params=pltpu.CompilerParams(
            vmem_limit_bytes=VMEM_LIMIT, collective_id=0, has_side_effects=True),
    )(coupling, lists, *inputs)


def per_device(charge_a, charge_b, coupling, positions, grid_base, spline, spline_slope, influence,
               pair_tiles, ghost_lists):
    group = lax.axis_size("px")
    reciprocal, real_space = run_step(
        group, coupling, pair_tiles.T, charge_a[None], charge_b[None], positions, grid_base, spline,
        spline_slope, ghost_lists, influence[:, 0])
    return reciprocal + real_space


def solution(mesh):
    placed = (
        P(("win", "px")),
        P(("win", "px")),
        P("win"),
        P(None, ("win", "px")),
        P(None, ("win", "px")),
        P(None, None, ("win", "px")),
        P(None, None, ("win", "px")),
        P(None, "px", None),
        P(("win", "px"), None),
        P(None, ("win", "px")),
    )
    return jax.shard_map(
        per_device, mesh=mesh, in_specs=placed, out_specs=P(None, ("win", "px")), check_vma=False
    )
```

```python
import functools
import math
import numpy as np
import jax
import jax.numpy as jnp
from jax import lax
from jax.experimental import pallas as pl
from jax.experimental.pallas import tpu as pltpu
from jax.sharding import PartitionSpec as P

TILE = 128
beta = 0.35
soften_sq = 0.25
VMEM_LIMIT = 60 * 1024 * 1024


def low_part(value):
    return value - value.astype(jnp.bfloat16).astype(jnp.float32)


def three_parts(value):
    first = value.astype(jnp.bfloat16).astype(jnp.float32)
    rest = value - first
    second = rest.astype(jnp.bfloat16).astype(jnp.float32)
    return first, second, rest - second


def dot(left, right, dims=((1,), (0,))):
    return lax.dot_general(left, right, (dims, ((), ())), preferred_element_type=jnp.float32)


def dot3(left, right):
    return dot(left, right) + (dot(low_part(left), right) + dot(left, low_part(right)))


def spline_columns(base_row, weights, length):
    lanes = base_row.shape[1]
    cells = lax.broadcasted_iota(jnp.int32, (length, lanes), 0)
    offset = (cells - base_row) & (length - 1)
    results = []
    for table in weights:
        value = jnp.zeros((length, lanes), jnp.float32)
        for step in reversed(range(len(table))):
            value = jnp.where(offset == step, table[step], value)
        results.append(value)
    return results


def dft_tables(length):
    index = np.arange(length)
    angle = 2.0 * np.pi * ((index[:, None] * index[None, :]) % length) / length
    cosine, sine = np.cos(angle), np.sin(angle)
    forward = np.block([[cosine, -sine], [sine, cosine]]).astype(np.float32)
    return forward, np.ascontiguousarray(forward.T)


def sum_tiles(value):
    rows, lanes = value.shape
    return jnp.sum(value.reshape(rows // 8, 8, lanes), axis=0)


def pair_features(scaled, home):
    first, second, third = three_parts(scaled)
    square = jnp.sum(scaled * scaled, axis=0, keepdims=True)
    ones = jnp.ones_like(square)
    if home:
        square = three_parts(square + soften_sq * beta * beta)
        rows = [first, first, second, second, first, third, *square, ones, ones, ones]
    else:
        square = three_parts(square)
        rows = [-2.0 * part for part in (first, second, first, second, third, first)]
        rows = rows + [ones, ones, ones, *square]
    rows.append(jnp.zeros((8, scaled.shape[1]), jnp.float32))
    return jnp.concatenate(rows, axis=0)


def pair_place(rows, shift, first_tile, near_table, source_table, home_table):
    local = jnp.concatenate([rows[0:1] + (shift - 0.5), rows[1:3] - 4.0], axis=0)
    scaled = local * beta
    q_a, q_b = rows[3:4], rows[4:5]
    source = jnp.concatenate([q_a, q_a * local, q_b, q_b * local], axis=0)
    source = jnp.concatenate([*three_parts(source), jnp.zeros_like(source)], axis=0)
    near = pair_features(scaled, False)
    near = jnp.concatenate([near, near, jnp.zeros((64, rows.shape[1]), jnp.float32)], axis=0)
    home = None if home_table is None else pair_features(scaled, True)
    for tile in range(rows.shape[1] // TILE):
        part = slice(tile * TILE, (tile + 1) * TILE)
        near_table[first_tile + tile] = near[:, part].T
        source_table[first_tile + tile] = source[:, part]
        if home is not None:
            home_table[first_tile + tile] = home[:, part]


def pair_own(slab_start, packet_ref, near_table, source_table, home_table, width=512):
    def own(step, carry):
        at = pl.ds(pl.multiple_of(step * width, width), width)
        pair_place(packet_ref[:, at], -slab_start, step * (width // TILE), near_table, source_table,
                   home_table)
        return carry

    lax.fori_loop(0, packet_ref.shape[1] // width, own, 0)


def pair_ghosts(slab_start, length, left_ref, right_ref, is_first, is_last, tiles, near_table,
                source_table):
    extra = left_ref.shape[1] // TILE
    pair_place(left_ref[...], -slab_start - is_first * length, tiles, near_table, source_table, None)
    pair_place(right_ref[...], -slab_start + is_last * length, tiles + extra, near_table,
               source_table, None)


def pair_tile(tile, packet_ref, slab_start, weight_b, lists_ref, near_table, source_table, home_table,
              out_ref):
    slots = lists_ref.shape[0]
    at = pl.ds(pl.multiple_of(tile * TILE, TILE), TILE)
    home = home_table[tile]
    blank = jnp.zeros_like(home)
    rest = jnp.zeros((TILE - 2 * home.shape[0], 2 * TILE), jnp.float32)
    wide_home = jnp.concatenate(
        [jnp.concatenate([home, blank], axis=1), jnp.concatenate([blank, home], axis=1), rest], axis=0)
    lane = lax.broadcasted_iota(jnp.int32, (TILE, TILE), 1)
    total = jnp.zeros((32, 2 * TILE), jnp.float32)
    for slot in range(0, slots, 2):
        one, two = lists_ref[slot, tile], lists_ref[slot + 1, tile]
        near = jnp.where(lane < 32, near_table[one], near_table[two])
        source = jnp.concatenate([source_table[one], source_table[two]], axis=1)
        square = dot(near, wide_home)
        inverse = lax.rsqrt(square)
        tail = (1.0 - lax.erf(square * inverse)) * inverse
        gauss = jnp.exp2(square * (-1.0 / math.log(2.0))) * (2.0 / math.sqrt(math.pi))
        radial = (tail + gauss) * (inverse * inverse)
        low = low_part(radial)
        both = jnp.concatenate(
            [jnp.concatenate([radial[:, :TILE], low[:, :TILE]], axis=1),
             jnp.concatenate([radial[:, TILE:], low[:, TILE:]], axis=1)], axis=0)
        total = total + dot(source, both)
    sums = total[:, :TILE] + total[:, TILE:]
    sums = sums[0:8] + sums[8:16] + sums[16:24]
    rows = packet_ref[:, at]
    local = jnp.concatenate([rows[0:1] - (slab_start + 0.5), rows[1:3] - 4.0], axis=0)
    scale = beta ** 3
    part_a = local * sums[0:1] - sums[1:4]
    part_b = local * sums[4:5] - sums[5:8]
    out_ref[:, at] = (
        ((1.0 - weight_b) * scale) * rows[3:4] * part_a + (weight_b * scale) * rows[4:5] * part_b)


VM = pl.BlockSpec(memory_space=pltpu.VMEM)
SM = pl.BlockSpec(memory_space=pltpu.SMEM)
params = pltpu.CompilerParams(vmem_limit_bytes=VMEM_LIMIT)


def f32(*shape):
    return jax.ShapeDtypeStruct(shape, jnp.float32)


def spread_atoms(chunk, charge_refs, base_ref, spline_ref, spread_out, grid_sum):
    order, _, full_y, full_z = spread_out.shape
    grid_sum[...] = jnp.zeros_like(grid_sum)

    def body(step, carry):
        at = pl.ds(pl.multiple_of(step * chunk, chunk), chunk)
        base = base_ref[:, at]
        weights = spline_ref[:, :, at]
        rows_y, = spline_columns(base[1:2], [[weights[1, o][None] for o in range(order)]], full_y)
        rows_z, = spline_columns(base[2:3], [[weights[2, o][None] for o in range(order)]], full_z)
        left = jnp.concatenate([ref[:, at] * rows_y for ref in charge_refs], axis=0)
        right = jnp.concatenate([weights[0, layer][None] * rows_z for layer in range(order)], axis=0)
        high = dot(jnp.concatenate([left, low_part(left)], axis=0), right, ((1,), (1,)))
        rest = dot(left, low_part(right), ((1,), (1,)))
        grid_sum[...] += high[:2 * full_y] + high[2 * full_y:] + rest
        return carry

    lax.fori_loop(0, base_ref.shape[1] // chunk, body, 0)
    for state in range(2):
        for layer in range(order):
            spread_out[layer, state] = grid_sum[state * full_y:(state + 1) * full_y,
                                                layer * full_z:(layer + 1) * full_z]


def gather_prepare(chunk, weight_b, charge_refs, base_ref, spline_ref, slope_ref, rows_y_ref,
                   slope_y_ref, wide_ref, low_ref, first, last):
    full_y = rows_y_ref.shape[0]
    order = spline_ref.shape[1]

    def body(step, carry):
        at = pl.ds(pl.multiple_of(step * chunk, chunk), chunk)
        twice = pl.ds(pl.multiple_of(step * 2 * chunk, 2 * chunk), 2 * chunk)
        base = base_ref[:, at]
        weights = spline_ref[:, :, at]
        slopes = slope_ref[:, :, at]

        def both(axis):
            return spline_columns(
                base[axis:axis + 1],
                [[table[axis, o][None] for o in range(order)] for table in (weights, slopes)],
                full_y)

        rows_y_ref[:, at], slope_y_ref[:, at] = both(1)
        stacked_z = jnp.concatenate(both(2), axis=1)
        scales = [(weight_b - 1.0) * charge_refs[0][:, at], -weight_b * charge_refs[1][:, at]]
        wide = jnp.concatenate(
            [jnp.concatenate([scale, scale], axis=1) * stacked_z for scale in scales], axis=0)
        wide_ref[:, twice] = wide
        low_ref[:, twice] = low_part(wide)
        return carry

    lax.fori_loop(first, last, body, 0)


def gather_layers(chunk, unroll, layers, before, spline_ref, slope_ref, plane_ref, rows_y_ref, slope_y_ref,
                  wide_ref, low_ref, out_ref, planes):
    _, _, full_y, full_z = plane_ref.shape
    height = len(layers) * full_y
    top = before * 2 * full_y
    for state in range(2):
        lanes = slice(state * full_z, (state + 1) * full_z)
        for place, layer in enumerate(layers):
            value = plane_ref[layer, state]
            first = top + place * full_y
            planes[first:first + full_y, lanes] = value
            planes[first + height:first + height + full_y, lanes] = low_part(value)

    def body(step, carry):
        at = pl.ds(pl.multiple_of(step * chunk, chunk), chunk)
        twice = pl.ds(pl.multiple_of(step * 2 * chunk, 2 * chunk), 2 * chunk)
        weights = spline_ref[0, :, at]
        slopes = slope_ref[0, :, at]
        rows_y, slope_y = rows_y_ref[:, at], slope_y_ref[:, at]
        high = dot(planes[top:top + 2 * height, :], wide_ref[:, twice])
        rest = dot(planes[top:top + height, :], low_ref[:, twice])
        sums = [jnp.zeros((8, chunk), jnp.float32) for _ in range(3)]
        for place, layer in enumerate(layers):
            part = slice(place * full_y, (place + 1) * full_y)
            again = slice(height + place * full_y, height + (place + 1) * full_y)
            sampled = high[part] + high[again] + rest[part]
            plain, sloped = sampled[:, :chunk], sampled[:, chunk:]
            plain_x, slope_x = weights[layer:layer + 1], slopes[layer:layer + 1]
            sums[0] = sums[0] + slope_x * sum_tiles(plain * rows_y)
            sums[1] = sums[1] + plain_x * sum_tiles(plain * slope_y)
            sums[2] = sums[2] + plain_x * sum_tiles(sloped * rows_y)
        for axis in range(3):
            result = jnp.sum(sums[axis], axis=0, keepdims=True)
            if before:
                result = result + out_ref[axis:axis + 1, at]
            out_ref[axis:axis + 1, at] = result
        return carry

    lax.fori_loop(0, spline_ref.shape[2] // chunk, body, 0, unroll=unroll)

MESH = pl.DeviceIdType.MESH
ATOMS_AT_ONCE = 512


def each(first, last, body, width):
    head = (last - first) % width
    for step in range(head):
        body(first + step)

    def block(index, carry):
        for step in range(width):
            body(first + head + index * width + step)
        return carry

    lax.fori_loop(0, (last - first - head) // width, block, 0)


def pick_ghosts(chunk, packet_ref, ghost_ref, ghost_out):
    height, atoms = packet_ref.shape
    ghosts = ghost_ref.shape[1]

    def pick(step, carry):
        at = pl.ds(pl.multiple_of(step * chunk, chunk), chunk)
        parts = jnp.concatenate(three_parts(packet_ref[:, at]), axis=0)
        ids = lax.broadcasted_iota(jnp.int32, (chunk, ghosts), 0) + step * chunk
        results = []
        for side in range(2):
            chosen = jnp.where(ids == ghost_ref[side:side + 1, :], 1.0, 0.0)
            results.append(carry[side] + dot(parts, chosen))
        return tuple(results)

    start = jnp.zeros((3 * height, ghosts), jnp.float32)
    sides = lax.fori_loop(0, atoms // chunk, pick, (start, start))
    for side, value in enumerate(sides):
        ghost_out[side] = value[:height] + value[height:2 * height] + value[2 * height:]


def step_kernel(group, scale, coupling_ref, lists_ref, *refs):
    inputs, (out_ref, real_ref), held, refs = refs[:14], refs[14:16], refs[16:30], refs[30:]
    (charge_a_ref, charge_b_ref, base_ref, spline_ref, position_ref, ghost_ref, slope_ref, influence_ref,
     table_ref, tablet_ref, table_rows_ref, tablet_rows_ref, table_columns_ref, tablet_columns_ref) = held
    (input_sem, rows_y, slope_y, wide_z, low_z, packet_ref, grid_sum, planes, spread_out, near_in, far_out, far_in, ghost_out, ghost_in, there_cross, there_out, there_in,
     back_cross, back_out, back_in,
     plane_in, near_table, source_table, home_table,
     near_send, near_recv, far_send, far_recv, ghost_send, ghost_recv, cross_send, cross_recv, row_send, row_recv,
     row_own,
     plane_send, plane_recv) = refs
    loads = [pltpu.make_async_copy(src, dst, input_sem.at[index])
             for index, (src, dst) in enumerate(zip(inputs, held))]
    for copy in loads:
        copy.start()
    me = lax.axis_index("px")
    order, _, full_y, full_z = spread_out.shape
    full_x = influence_ref.shape[0]
    tiles = lists_ref.shape[1]
    slab_start = me.astype(jnp.float32)

    def other(steps):
        return {"px": lax.rem(me + (steps + group), group)}

    barrier = pltpu.get_barrier_semaphore()

    def greet(steps):
        pl.semaphore_signal(barrier, inc=1, device_id=other(steps), device_id_type=MESH)

    chips = group // 2
    half = chips // 2

    with jax.named_scope("greet"):
        greet(2 * half)

        def greet_both(steps):
            greet(2 * (half - steps))
            greet(2 * (half + steps))

        each(1, half, greet_both, 5)
        greet(1)
        greet(-1)

    charge_refs = (charge_a_ref, charge_b_ref)
    for copy in loads[:4]:
        copy.wait()
    with jax.named_scope("spread"):
        spread_atoms(2048, charge_refs, base_ref, spline_ref, spread_out, grid_sum)

    with jax.named_scope("barrier_wait"):
        pl.semaphore_wait(barrier, chips + 1)

    odd = lax.rem(me, 2)
    partner = other(1 - 2 * odd)

    def carry_to(device, src, dst, sends, recvs, at):
        return pltpu.make_async_remote_copy(
            src_ref=src, dst_ref=dst, send_sem=sends.at[at], recv_sem=recvs.at[at],
            device_id=device, device_id_type=MESH)

    third = [carry_to(other(1), spread_out.at[3, s], near_in.at[1, s], near_send, near_recv, 2 + s)
             for s in range(2)]
    first = [carry_to(partner, spread_out.at[1, s], near_in.at[0, s], near_send, near_recv, s)
             for s in range(2)]
    far = [carry_to(other(2), far_out.at[s], far_in.at[s], far_send, far_recv, s) for s in range(2)]
    visits = [carry_to(other(1 - 2 * side), ghost_out.at[side], ghost_in.at[side], ghost_send,
                       ghost_recv, side) for side in range(2)]
    for copy in third + first:
        copy.start()
    for copy in loads[4:7]:
        copy.wait()
    with jax.named_scope("pick"):
        packet_ref[0:3, :] = position_ref[...]
        packet_ref[3:4, :] = charge_a_ref[...]
        packet_ref[4:5, :] = charge_b_ref[...]
        packet_ref[5:8, :] = jnp.zeros_like(position_ref)
        pick_ghosts(512, packet_ref, ghost_ref, ghost_out)
    prepare = functools.partial(gather_prepare, ATOMS_AT_ONCE, coupling_ref[0], charge_refs, base_ref,
                                spline_ref, slope_ref, rows_y, slope_y, wide_z, low_z)
    for copy in visits:
        copy.start()
    with jax.named_scope("wait_near"):
        for s in range(2):
            first[s].wait()
            third[s].wait()
            far_out[s] = spread_out[2, s] + near_in[1, s] + jnp.where(odd == 0, near_in[0, s], 0.0)
            far[s].start()
    with jax.named_scope("prepare_a"):
        prepare(0, 2)
    with jax.named_scope("pair_own"):
        pair_own(slab_start, packet_ref, near_table, source_table, home_table)
    with jax.named_scope("prepare_b"):
        prepare(2, 6)
    with jax.named_scope("wait_far"):
        for copy in far:
            copy.wait()

    chip = lax.div(me, 2)

    def swap_rows(columns, cross, paired, in_rows, which):
        upper, lower = columns[:group], columns[group:]
        mine = jnp.where(odd == 0, upper, lower)
        theirs = jnp.where(odd == 0, lower, upper)
        for part in range(2):
            rows_at = slice(part * chips, (part + 1) * chips)
            cross[:, part, :] = theirs[rows_at]
            paired[:, odd, part, :] = mine[rows_at]
        over = carry_to(partner, cross, paired.at[:, odd], cross_send, cross_recv, which)
        over.start()

        def row_to(steps):
            return pltpu.make_async_remote_copy(
                src_ref=paired.at[lax.rem(chip + steps, chips)], dst_ref=in_rows.at[chip],
                send_sem=row_send.at[which], recv_sem=row_recv.at[which],
                device_id=other(2 * steps), device_id_type=MESH)

        own = pltpu.make_async_copy(paired.at[chip], in_rows.at[chip], row_own.at[which])

        def send(steps):
            row_to(half - steps).start()
            row_to(half + steps).start()

        def go():
            over.wait()
            own.start()
            row_to(half).start()
            each(1, half, send, 5)

        def finish():
            own.wait()
            every = pltpu.make_async_remote_copy(
                src_ref=paired.at[pl.ds(0, chips - 1)], dst_ref=in_rows.at[pl.ds(0, chips - 1)],
                send_sem=row_send.at[which], recv_sem=row_recv.at[which],
                device_id=other(2 * half), device_id_type=MESH)
            every.wait()
            return jnp.concatenate(
                [in_rows[:, side, part, :] for side in range(2) for part in range(2)], axis=0)

        return go, finish

    def pairs(first, last):
        def body(tile, carry):
            pair_tile(tile, packet_ref, slab_start, coupling_ref[0], lists_ref, near_table,
                      source_table, home_table, real_ref)
            return carry

        lax.fori_loop(first, last, body, 0, unroll=8)

    for copy in loads[7:]:
        copy.wait()
    value = spread_out[0] + far_in[...] + jnp.where(odd == 0, 0.0, near_in[0])
    rows = dot3(jnp.concatenate([value[0], value[1]], axis=1), table_ref[...])
    rows = jnp.concatenate([rows[:, :full_z], rows[:, full_z:]], axis=0)
    go, finish = swap_rows(dot3(tablet_rows_ref[...], rows), there_cross, there_out, there_in, 0)
    with jax.named_scope("send_there"):
        go()
    with jax.named_scope("ghosts"):
        for copy in visits:
            copy.wait()
        is_first = jnp.where(me == 0, 1.0, 0.0)
        is_last = jnp.where(me == group - 1, 1.0, 0.0)
        pair_ghosts(slab_start, float(full_x), ghost_in.at[0], ghost_in.at[1], is_first, is_last,
                    tiles, near_table, source_table)
    with jax.named_scope("pairs_a"):
        pairs(0, tiles // 2)
    with jax.named_scope("prepare_c"):
        prepare(6, base_ref.shape[1] // ATOMS_AT_ONCE)
    with jax.named_scope("wait_there"):
        columns = finish()

    columns = dot3(tablet_columns_ref[...], columns)
    gain = influence_ref[...] * scale
    columns = dot3(table_rows_ref[...], columns * jnp.concatenate([gain, gain], axis=0))
    go, finish = swap_rows(columns, back_cross, back_out, back_in, 1)
    with jax.named_scope("send_back"):
        go()
    with jax.named_scope("pairs_b"):
        pairs(tiles // 2, tiles)
    with jax.named_scope("wait_back"):
        columns = finish()

    columns = dot3(table_columns_ref[...], columns)
    rows = dot3(jnp.concatenate([columns[:full_y], columns[full_y:]], axis=1), tablet_ref[...])
    plane_in[0, 0] = rows[:, :full_z]
    plane_in[0, 1] = rows[:, full_z:]
    lend_two = [carry_to(other(-2), plane_in.at[0, s], plane_in.at[2, s], plane_send, plane_recv, s)
                for s in range(2)]
    lend_three = [carry_to(other(-1), plane_in.at[2, s], plane_in.at[3, s], plane_send, plane_recv,
                           2 + s) for s in range(2)]
    lend_one, pass_one = (
        [carry_to(partner, plane_in.at[at, s], plane_in.at[1, s], plane_send, plane_recv, 4 + s)
         for s in range(2)] for at in (0, 2))
    for copy in lend_two:
        copy.start()

    @pl.when(odd == 1)
    def _():
        for copy in lend_one:
            copy.start()

    def gather(layers, before):
        gather_layers(ATOMS_AT_ONCE, 4 // len(layers), layers, before, spline_ref, slope_ref, plane_in,
                      rows_y, slope_y, wide_z, low_z, out_ref, planes)

    with jax.named_scope("gather_a"):
        gather((0,), 0)
    with jax.named_scope("wait_two"):
        for s in range(2):
            lend_two[s].wait()
            lend_three[s].start()

            @pl.when(odd == 0)
            def _():
                pass_one[s].start()

    with jax.named_scope("gather_b"):
        gather((2,), 1)
    with jax.named_scope("wait_three"):
        for copy in lend_three + lend_one:
            copy.wait()
    with jax.named_scope("gather_c"):
        gather((1, 3), 2)


def run_step(group, coupling, lists, charge_a, charge_b, positions, grid_base, spline, slope, ghosts,
             influence):
    order = spline.shape[1]
    full_x, full_z = influence.shape
    full_y = group
    atoms = positions.shape[1]
    tiles = lists.shape[1]
    visitors = ghosts.shape[1]
    every = tiles + 2 * (visitors // TILE)
    plane = (2, full_y, full_z)
    tables = dft_tables(full_x)
    order_of = np.arange(full_x)
    sides = [order_of[side::2] + part * full_x for side in range(2) for part in range(2)]
    split = np.concatenate(sides)
    tables = tables + tuple(value[split] for value in tables) + tuple(value[:, split] for value in tables)
    inputs = (charge_a, charge_b, grid_base, spline, positions, ghosts, slope, influence,
              *(jnp.asarray(value) for value in tables))
    return pl.pallas_call(
        functools.partial(step_kernel, group, 1.0 / (full_x * full_y * full_z)),
        out_shape=[f32(3, atoms)] * 2,
        in_specs=[SM] * 2 + [pl.BlockSpec(memory_space=pl.ANY)] * len(inputs),
        out_specs=[VM] * 2,
        scratch_shapes=[pltpu.VMEM(value.shape, value.dtype) for value in inputs] + [
            pltpu.SemaphoreType.DMA((len(inputs),)),
            pltpu.VMEM((full_y, atoms), jnp.float32),
            pltpu.VMEM((full_y, atoms), jnp.float32),
            pltpu.VMEM((2 * full_z, 2 * atoms), jnp.float32),
            pltpu.VMEM((2 * full_z, 2 * atoms), jnp.float32),
            pltpu.VMEM((8, atoms), jnp.float32),
            pltpu.VMEM((2 * full_y, order * full_z), jnp.float32),
            pltpu.VMEM((2 * order * full_y, 2 * full_z), jnp.float32),
            pltpu.VMEM((order, *plane), jnp.float32),
            pltpu.VMEM((2, *plane), jnp.float32),
            pltpu.VMEM(plane, jnp.float32),
            pltpu.VMEM(plane, jnp.float32),
            pltpu.VMEM((2, 8, visitors), jnp.float32),
            pltpu.VMEM((2, 8, visitors), jnp.float32),
            *[pltpu.VMEM((group // 2, *sides, 2, full_z), jnp.float32)
              for sides in ((), (2,), (2,)) * 2],
            pltpu.VMEM((order, *plane), jnp.float32),
            pltpu.VMEM((every, TILE, TILE), jnp.float32),
            pltpu.VMEM((every, 32, TILE), jnp.float32),
            pltpu.VMEM((tiles, 32, TILE), jnp.float32),
            *[pltpu.SemaphoreType.DMA((count,)) for count in (4, 4, 2, 2, 2, 2, 2, 2, 2, 2, 2, 6, 6)],
        ],
        compiler_params=pltpu.CompilerParams(
            vmem_limit_bytes=VMEM_LIMIT, collective_id=0, has_side_effects=True),
    )(coupling, lists, *inputs)


def per_device(charge_a, charge_b, coupling, positions, grid_base, spline, spline_slope, influence,
               pair_tiles, ghost_lists):
    group = lax.axis_size("px")
    reciprocal, real_space = run_step(
        group, coupling, pair_tiles.T, charge_a[None], charge_b[None], positions, grid_base, spline,
        spline_slope, ghost_lists, influence[:, 0])
    return reciprocal + real_space


def solution(mesh):
    placed = (
        P(("win", "px")),
        P(("win", "px")),
        P("win"),
        P(None, ("win", "px")),
        P(None, ("win", "px")),
        P(None, None, ("win", "px")),
        P(None, None, ("win", "px")),
        P(None, "px", None),
        P(("win", "px"), None),
        P(None, ("win", "px")),
    )
    return jax.shard_map(
        per_device, mesh=mesh, in_specs=placed, out_specs=P(None, ("win", "px")), check_vma=False
    )
```
